8 devices in a mesh: tp: 8 (over z, y, x, core).
Axes of the slice: x: 2, y: 2, z: 1, core: 2. Of those that a mesh axis runs over, the one named last changes fastest.
Arguments:
- x_in: bfloat16 [16, 256, 2560], P(None, 'tp')
- grad_y: bfloat16 [16, 256, 2560], P(None, 'tp')
- ln_gain: float32 [2560], replicated
- w_query: bfloat16 [2560, 32, 80], P(None, 'tp')
- w_key: bfloat16 [2560, 80], replicated
- w_value: bfloat16 [2560, 80], replicated
- w_out: bfloat16 [32, 80, 2560], P('tp')
- w_gate: bfloat16 [2560, 10240], P(None, 'tp')
- w_up: bfloat16 [2560, 10240], P(None, 'tp')
- w_down: bfloat16 [10240, 2560], P('tp')
Outputs:
- output 1: bfloat16 [16, 256, 2560], P(None, 'tp')
- output 2: bfloat16 [16, 256, 2560], P(None, 'tp')
- output 3: float32 [2560], replicated
- output 4: bfloat16 [2560, 32, 80], P(None, 'tp')
- output 5: bfloat16 [2560, 80], replicated
- output 6: bfloat16 [2560, 80], replicated
- output 7: bfloat16 [32, 80, 2560], P('tp')
- output 8: bfloat16 [2560, 10240], P(None, 'tp')
- output 9: bfloat16 [2560, 10240], P(None, 'tp')
- output 10: bfloat16 [10240, 2560], P('tp')
All inputs are finite; a program needn't handle non-finite values.
Results may differ from the reference program's by a relative error of at most 0.0155186.
Values are sent between devices in bfloat16 or wider.
A program may use at most 1 GiB of HBM per device.

```python
import jax
import jax.numpy as jnp
from jax import lax

BATCH_SIZE = 16
SEQ_LEN = 256
MODEL_DIM = 2560
NUM_HEADS = 32
HEAD_DIM = 80
FFN_DIM = 10240

LN_EPS = 1e-6
ROPE_BASE = 10000.0


def setup_inputs(seed: int = 0) -> dict:
    keys = jax.random.split(jax.random.key(seed), 12)
    act_shape = (BATCH_SIZE, SEQ_LEN, MODEL_DIM)
    mean_vec = jax.random.normal(keys[0], (MODEL_DIM,), jnp.float32)
    tok_scale = jnp.exp(jax.random.uniform(keys[1], (BATCH_SIZE, SEQ_LEN, 1), jnp.float32, -0.7, 0.7))
    x_in = (jax.random.normal(keys[2], act_shape, jnp.float32) + mean_vec) * tok_scale
    grad_y = jax.random.normal(keys[3], act_shape, jnp.float32)
    ln_gain = jax.random.uniform(keys[4], (MODEL_DIM,), jnp.float32, 0.2, 2.0)
    in_scale = MODEL_DIM ** -0.5
    w_query = jax.random.normal(keys[5], (MODEL_DIM, NUM_HEADS, HEAD_DIM), jnp.float32) * in_scale
    w_key = jax.random.normal(keys[6], (MODEL_DIM, HEAD_DIM), jnp.float32) * in_scale
    w_value = jax.random.normal(keys[7], (MODEL_DIM, HEAD_DIM), jnp.float32) * in_scale
    w_out = jax.random.normal(keys[8], (NUM_HEADS, HEAD_DIM, MODEL_DIM), jnp.float32) * (NUM_HEADS * HEAD_DIM) ** -0.5
    w_gate = jax.random.normal(keys[9], (MODEL_DIM, FFN_DIM), jnp.float32) * in_scale
    w_up = jax.random.normal(keys[10], (MODEL_DIM, FFN_DIM), jnp.float32) * in_scale
    w_down = jax.random.normal(keys[11], (FFN_DIM, MODEL_DIM), jnp.float32) * FFN_DIM ** -0.5
    return {
        "x_in": x_in.astype(jnp.bfloat16),
        "grad_y": grad_y.astype(jnp.bfloat16),
        "ln_gain": ln_gain,
        "w_query": w_query.astype(jnp.bfloat16),
        "w_key": w_key.astype(jnp.bfloat16),
        "w_value": w_value.astype(jnp.bfloat16),
        "w_out": w_out.astype(jnp.bfloat16),
        "w_gate": w_gate.astype(jnp.bfloat16),
        "w_up": w_up.astype(jnp.bfloat16),
        "w_down": w_down.astype(jnp.bfloat16),
    }


def as_bf16(value):
    return value + lax.stop_gradient(value.astype(jnp.bfloat16).astype(jnp.float32) - value)


def rope_tables(seq_len, head_dim):
    half_dim = head_dim // 2
    inv_freq = ROPE_BASE ** (-jnp.arange(half_dim, dtype=jnp.float32) * 2.0 / head_dim)
    angles = jnp.arange(seq_len, dtype=jnp.float32)[:, None] * inv_freq[None, :]
    return jnp.cos(angles), jnp.sin(angles)


def rotate_half(values, cos_tab, sin_tab):
    half_dim = values.shape[-1] // 2
    first_half = values[..., :half_dim]
    second_half = values[..., half_dim:]
    return jnp.concatenate([first_half * cos_tab - second_half * sin_tab, second_half * cos_tab + first_half * sin_tab], axis=-1)


def layer_forward(x_in, ln_gain, w_query, w_key, w_value, w_out, w_gate, w_up, w_down):
    residual = x_in.astype(jnp.float32)
    centered = residual - jnp.mean(residual, axis=-1, keepdims=True)
    inv_std = lax.rsqrt(jnp.mean(centered * centered, axis=-1, keepdims=True) + LN_EPS)
    normed = as_bf16(ln_gain * centered * inv_std)
    cos_tab, sin_tab = rope_tables(SEQ_LEN, HEAD_DIM)
    q_raw = jnp.einsum("bld,dnk->blnk", normed, w_query.astype(jnp.float32))
    k_raw = jnp.einsum("bld,dk->blk", normed, w_key.astype(jnp.float32))
    values = as_bf16(jnp.einsum("bld,dk->blk", normed, w_value.astype(jnp.float32)))
    q_rot = as_bf16(rotate_half(q_raw, cos_tab[:, None, :], sin_tab[:, None, :]))
    k_rot = as_bf16(rotate_half(k_raw, cos_tab, sin_tab))
    scores = jnp.einsum("bqnk,bsk->bnqs", q_rot, k_rot) * HEAD_DIM ** -0.5
    positions = jnp.arange(SEQ_LEN)
    causal = positions[:, None] >= positions[None, :]
    attn_probs = as_bf16(jax.nn.softmax(jnp.where(causal, scores, -1e30), axis=-1))
    attn_heads = as_bf16(jnp.einsum("bnqs,bsk->bqnk", attn_probs, values))
    attn_out = jnp.einsum("bqnk,nkd->bqd", attn_heads, w_out.astype(jnp.float32))
    gate_pre = jnp.einsum("bld,df->blf", normed, w_gate.astype(jnp.float32))
    up_pre = jnp.einsum("bld,df->blf", normed, w_up.astype(jnp.float32))
    hidden = as_bf16(jax.nn.silu(gate_pre) * up_pre)
    mlp_out = jnp.einsum("blf,fd->bld", hidden, w_down.astype(jnp.float32))
    return residual + attn_out + mlp_out


def reference(x_in, grad_y, ln_gain, w_query, w_key, w_value, w_out, w_gate, w_up, w_down):
    out_f32, pullback = jax.vjp(layer_forward, x_in, ln_gain, w_query, w_key, w_value, w_out, w_gate, w_up, w_down)
    gradients = pullback(grad_y.astype(jnp.float32))
    return (
        out_f32.astype(jnp.bfloat16),
        gradients[0].astype(jnp.bfloat16),
        gradients[1].astype(jnp.float32),
        gradients[2].astype(jnp.bfloat16),
        gradients[3].astype(jnp.bfloat16),
        gradients[4].astype(jnp.bfloat16),
        gradients[5].astype(jnp.bfloat16),
        gradients[6].astype(jnp.bfloat16),
        gradients[7].astype(jnp.bfloat16),
        gradients[8].astype(jnp.bfloat16),
    )
```

```python
import functools

import jax
import jax.numpy as jnp
from jax import lax
from jax.experimental import pallas as pl
from jax.experimental.pallas import tpu as pltpu
from jax.sharding import PartitionSpec as P

LN_EPS = 1e-6
ROPE_BASE = 10000.0
BF = jnp.bfloat16
F32 = jnp.float32
CHUNKS = 2
VMEM_LIMIT = 60 * 1024 * 1024
NT_DIMS = (((1,), (1,)), ((), ()))


def rope_tables(seq_len, head_dim):
    half_dim = head_dim // 2
    inv_freq = ROPE_BASE ** (-jnp.arange(half_dim, dtype=F32) * 2.0 / head_dim)
    angles = jnp.arange(seq_len, dtype=F32)[:, None] * inv_freq[None, :]
    return jnp.cos(angles).T, jnp.sin(angles).T


def rotate(values, cos_tab, sin_tab):
    half = values.shape[0] // 2
    first, second = values[:half], values[half:]
    return jnp.concatenate([first * cos_tab - second * sin_tab, second * cos_tab + first * sin_tab], axis=0)


def attn_fwd_kernel(heads, scale, qkv_ref, cos_ref, sin_ref, o_ref, rot_ref, stat_ref):
    hd = 2 * cos_ref.shape[0]
    cos, sin = cos_ref[...], sin_ref[...]
    seq = cos.shape[1]
    k_t = rotate(qkv_ref[0, heads * hd:(heads + 1) * hd], cos, sin)
    v_t = qkv_ref[0, (heads + 1) * hd:].astype(BF)
    rot_ref[0, heads * hd:(heads + 1) * hd] = k_t.astype(BF)
    rot_ref[0, (heads + 1) * hd:] = v_t
    k = k_t.T.astype(BF)
    causal = lax.broadcasted_iota(jnp.int32, (seq, seq), 0) <= lax.broadcasted_iota(jnp.int32, (seq, seq), 1)
    outs = []
    for n in range(heads):
        q_t = rotate(qkv_ref[0, n * hd:(n + 1) * hd], cos, sin).astype(BF)
        rot_ref[0, n * hd:(n + 1) * hd] = q_t
        scores = jnp.dot(k, q_t, preferred_element_type=F32) * scale
        scores = jnp.where(causal, scores, -1e30)
        top = jnp.max(scores, axis=0, keepdims=True)
        expd = jnp.exp(scores - top)
        inv = 1.0 / jnp.sum(expd, axis=0, keepdims=True)
        stat_ref[0, n:n + 1] = top
        stat_ref[0, heads + n:heads + n + 1] = inv
        probs = (expd * inv).astype(BF)
        outs.append(jnp.dot(v_t, probs, preferred_element_type=F32))
    o_ref[0] = jnp.concatenate(outs, axis=0).T.astype(BF)


def attn_bwd_kernel(heads, scale, rot_ref, do_ref, stat_ref, cos_ref, sin_ref, dqkv_ref):
    hd = 2 * cos_ref.shape[0]
    cos, sin = cos_ref[...], sin_ref[...]
    seq = cos.shape[1]
    k_t = rot_ref[0, heads * hd:(heads + 1) * hd]
    v_t = rot_ref[0, (heads + 1) * hd:]
    k = k_t.astype(F32).T.astype(BF)
    v = v_t.astype(F32).T.astype(BF)
    causal = lax.broadcasted_iota(jnp.int32, (seq, seq), 0) <= lax.broadcasted_iota(jnp.int32, (seq, seq), 1)
    grads = []
    dk_t = jnp.zeros((hd, seq), F32)
    dv_t = jnp.zeros((hd, seq), F32)
    for n in range(heads):
        q_t = rot_ref[0, n * hd:(n + 1) * hd]
        do_t = do_ref[0, n * hd:(n + 1) * hd]
        scores = jnp.dot(k, q_t, preferred_element_type=F32) * scale
        scores = jnp.where(causal, scores, -1e30)
        probs = jnp.exp(scores - stat_ref[0, n:n + 1]) * stat_ref[0, heads + n:heads + n + 1]
        dprobs = jnp.dot(v, do_t, preferred_element_type=F32)
        row_dot = jnp.sum(probs * dprobs, axis=0, keepdims=True)
        dscores = (probs * (dprobs - row_dot) * scale).astype(BF)
        grads.append(rotate(jnp.dot(k_t, dscores, preferred_element_type=F32), cos, -sin))
        dk_t += lax.dot_general(q_t, dscores, NT_DIMS, preferred_element_type=F32)
        dv_t += lax.dot_general(do_t, probs.astype(BF), NT_DIMS, preferred_element_type=F32)
    grads += [rotate(dk_t, cos, -sin), dv_t]
    dqkv_ref[0] = jnp.concatenate(grads, axis=0).T.astype(BF)


def attn_fwd(qkv_t, cos, sin, heads):
    batch, rows, seq = qkv_t.shape
    hd = rows // (heads + 2)
    block = lambda r, c: pl.BlockSpec((1, r, c), lambda b: (b, 0, 0))
    table = pl.BlockSpec(cos.shape, lambda b: (0, 0))
    return pl.pallas_call(
        functools.partial(attn_fwd_kernel, heads, hd ** -0.5),
        grid=(batch,),
        out_shape=(
            jax.ShapeDtypeStruct((batch, seq, heads * hd), BF),
            jax.ShapeDtypeStruct((batch, rows, seq), BF),
            jax.ShapeDtypeStruct((batch, 2 * heads, seq), F32),
        ),
        in_specs=[block(rows, seq), table, table],
        out_specs=(block(seq, heads * hd), block(rows, seq), block(2 * heads, seq)),
        compiler_params=pltpu.CompilerParams(vmem_limit_bytes=32 * 1024 * 1024),
        cost_estimate=pl.CostEstimate(flops=batch * 10_000_000_00, bytes_accessed=batch * rows * seq * 8, transcendentals=0),
        name="attn_fwd",
    )(qkv_t, cos, sin)


def attn_bwd(rot, do_t, stat, cos, sin, heads):
    batch, rows, seq = rot.shape
    hd = rows // (heads + 2)
    block = lambda r, c: pl.BlockSpec((1, r, c), lambda b: (b, 0, 0))
    table = pl.BlockSpec(cos.shape, lambda b: (0, 0))
    return pl.pallas_call(
        functools.partial(attn_bwd_kernel, heads, hd ** -0.5),
        grid=(batch,),
        out_shape=jax.ShapeDtypeStruct((batch, seq, rows), BF),
        in_specs=[block(rows, seq), block(heads * hd, seq), block(2 * heads, seq), table, table],
        out_specs=block(seq, rows),
        compiler_params=pltpu.CompilerParams(vmem_limit_bytes=32 * 1024 * 1024),
        cost_estimate=pl.CostEstimate(flops=batch * 20_000_000_00, bytes_accessed=batch * rows * seq * 6, transcendentals=0),
        name="attn_bwd",
    )(rot, do_t, stat, cos, sin)


def pair_matmul_kernel(num, trans, tiles, *refs):
    a_hbm, b_refs, out_ref = refs[:num], refs[num:2 * num], refs[2 * num]
    a_vmem = refs[2 * num + 1:3 * num + 1]
    send_buf, recv_buf, a_sem, send_sem, recv_sem = refs[3 * num + 1:]
    step = pl.program_id(0)
    me = lax.axis_index("tp")
    core = lax.rem(me, 2)
    partner = me + 1 - 2 * core
    chips = a_vmem[0].shape[1]

    def load(half, which, chip):
        parity = 1 - core if half == 0 else core
        return pltpu.make_async_copy(a_hbm[which].at[:, chip, parity], a_vmem[which].at[half, chip], a_sem.at[half, which, chip])

    def exchange(tile):
        return pltpu.make_async_remote_copy(
            src_ref=send_buf.at[tile], dst_ref=recv_buf.at[tile], send_sem=send_sem.at[tile], recv_sem=recv_sem.at[tile],
            device_id=(partner,), device_id_type=pl.DeviceIdType.MESH)

    def product(half, rows):
        total = None
        for which in range(num):
            lhs = a_vmem[which][half, rows]
            lhs = lhs.reshape(-1, lhs.shape[-1])
            rhs = b_refs[which][...]
            term = lax.dot_general(lhs, rhs, NT_DIMS, preferred_element_type=F32) if trans[which] else jnp.dot(lhs, rhs, preferred_element_type=F32)
            total = term if total is None else total + term
        return total

    group = 2
    shape = (group,) + send_buf.shape[2:]

    @pl.when(step == 0)
    def _():
        for half in range(2):
            for which in range(num):
                for chip in range(chips):
                    load(half, which, chip).start()
        barrier = pltpu.get_barrier_semaphore()
        pl.semaphore_signal(barrier, inc=1, device_id=(partner,), device_id_type=pl.DeviceIdType.MESH)
        pl.semaphore_wait(barrier, 1)
        for which in range(num):
            for chip in range(chips):
                load(0, which, chip).wait()

    for tile in range(tiles):
        @pl.when(step == tile + 1)
        def _():
            exchange(tile).start()

    @pl.when(step == tiles)
    def _():
        for which in range(num):
            for chip in range(chips):
                load(1, which, chip).wait()

    for tile in range(tiles):
        @pl.when(step == tile + tiles)
        def _():
            exchange(tile).wait_recv()

    @pl.when(step < tiles)
    def _():
        @pl.loop(0, chips // group)
        def _(g):
            rows = pl.ds(g * group, group)
            send_buf[step, rows] = product(0, rows).astype(BF).reshape(shape)

    @pl.when(step >= tiles)
    def _():
        @pl.loop(0, chips // group)
        def _(g):
            rows = pl.ds(g * group, group)
            arrived = recv_buf[step - tiles, rows].reshape(-1, shape[-1])
            out_ref[rows] = (product(1, rows) + arrived.astype(F32)).astype(BF).reshape(shape)

    @pl.when(step == 2 * tiles - 1)
    def _():
        for tile in range(tiles):
            exchange(tile).wait_send()


def pair_matmul(lhs, rhs, trans, collective_id, name, tile=512):
    num = len(lhs)
    batch, seq = lhs[0].shape[:2]
    chips, local = 4, seq // 8
    lhs = [a.reshape(batch, chips, 2, local, a.shape[-1]) for a in lhs]
    width = rhs[0].shape[0] if trans[0] else rhs[0].shape[1]
    tiles = width // tile
    in_specs = [pl.BlockSpec(memory_space=pl.ANY)] * num
    for b, t in zip(rhs, trans):
        if t:
            in_specs.append(pl.BlockSpec((tile, b.shape[1]), lambda i: (lax.rem(i, tiles), 0)))
        else:
            in_specs.append(pl.BlockSpec((b.shape[0], tile), lambda i: (0, lax.rem(i, tiles))))
    depth = sum(a.shape[-1] for a in lhs)
    return pl.pallas_call(
        functools.partial(pair_matmul_kernel, num, trans, tiles),
        grid=(2 * tiles,),
        out_shape=jax.ShapeDtypeStruct((chips, batch, local, width), BF),
        in_specs=in_specs,
        out_specs=pl.BlockSpec((chips, batch, local, tile), lambda i: (0, 0, 0, lax.max(i - tiles, 0))),
        scratch_shapes=[pltpu.VMEM((2, chips, batch, local, a.shape[-1]), BF) for a in lhs] + [
            pltpu.VMEM((tiles, chips, batch, local, tile), BF),
            pltpu.VMEM((tiles, chips, batch, local, tile), BF),
            pltpu.SemaphoreType.DMA((2, num, chips)),
            pltpu.SemaphoreType.DMA((tiles,)),
            pltpu.SemaphoreType.DMA((tiles,)),
        ],
        compiler_params=pltpu.CompilerParams(collective_id=collective_id, has_side_effects=True, vmem_limit_bytes=VMEM_LIMIT),
        cost_estimate=pl.CostEstimate(flops=2 * batch * seq * width * depth, bytes_accessed=2 * depth * (batch * seq + width), transcendentals=0),
        name=name,
    )(*lhs, *rhs)


def solution(mesh):
    group_size = mesh.shape["tp"]
    same_core = [[c + 2 * j for j in range(group_size // 2)] for c in range(2)]

    def layer_shard(x_loc, grad_y_loc, ln_gain, w_query, w_key, w_value, w_out, w_gate, w_up, w_down):
        head_dim = w_key.shape[1]
        heads = w_query.shape[1]
        width = x_loc.shape[2]
        seq_len = x_loc.shape[1] * group_size
        rows = x_loc.shape[0] // CHUNKS
        cos_tab, sin_tab = rope_tables(seq_len, head_dim)
        w_qkv_t = jnp.concatenate([w_query.transpose(1, 2, 0).reshape(heads * head_dim, width), w_key.T, w_value.T], axis=0)
        w_out_2d = w_out.reshape(heads * head_dim, width)

        def normalize(x):
            residual = x.astype(F32)
            centered = residual - jnp.mean(residual, axis=-1, keepdims=True)
            inv_std = lax.rsqrt(jnp.mean(centered * centered, axis=-1, keepdims=True) + LN_EPS)
            return residual, centered * inv_std, inv_std

        xs = [x_loc[c * rows:(c + 1) * rows] for c in range(CHUNKS)]
        dys = [grad_y_loc[c * rows:(c + 1) * rows] for c in range(CHUNKS)]
        sums = {k: 0.0 for k in ("qkv", "out", "gate", "up", "down")}
        ys, dhs = [], []
        saved = []
        for c in range(CHUNKS):
            normed_loc = (ln_gain * normalize(xs[c])[1]).astype(BF)
            normed = lax.all_gather(normed_loc, "tp", axis=1, tiled=True)
            grad = lax.all_gather(dys[c], "tp", axis=1, tiled=True)
            qkv_t = jnp.einsum("kd,bld->bkl", w_qkv_t, normed, preferred_element_type=F32)
            attn, rot, stat = attn_fwd(qkv_t, cos_tab, sin_tab, heads)
            gate_pre = jnp.einsum("bld,df->blf", normed, w_gate, preferred_element_type=F32)
            up_pre = jnp.einsum("bld,df->blf", normed, w_up, preferred_element_type=F32)
            gate_sig = jax.nn.sigmoid(gate_pre)
            gate_act = gate_pre * gate_sig
            hidden = (gate_act * up_pre).astype(BF)
            branch = pair_matmul([hidden, attn], [w_down, w_out_2d], (False, False), 1, "branch_mm")
            ys.append(lax.psum_scatter(branch, "tp", scatter_dimension=0, tiled=False, axis_index_groups=same_core))

            do_t = jnp.einsum("kd,bld->bkl", w_out_2d, grad, preferred_element_type=F32).astype(BF)
            grad_hidden = jnp.einsum("bld,fd->blf", grad, w_down, preferred_element_type=F32)
            grad_gate = (grad_hidden * up_pre * gate_sig * (1.0 + gate_pre * (1.0 - gate_sig))).astype(BF)
            grad_up = (grad_hidden * gate_act).astype(BF)
            dqkv = attn_bwd(rot, do_t, stat, cos_tab, sin_tab, heads)
            dh = pair_matmul([grad_gate, grad_up, dqkv], [w_gate, w_up, w_qkv_t], (True, True, False), 2, "dh_mm")
            dhs.append(lax.psum_scatter(dh, "tp", scatter_dimension=0, tiled=False, axis_index_groups=same_core))
            saved.append((normed, grad, hidden, attn, grad_gate, grad_up, dqkv))

        total = lambda spec, i, j: sum(jnp.einsum(spec, s[i], s[j], preferred_element_type=F32) for s in saved)
        dw_qkv = total("blk,bld->kd", 6, 0)
        dw_kv = lax.psum(dw_qkv[heads * head_dim:], "tp")
        dw_query = dw_qkv[:heads * head_dim].reshape(heads, head_dim, width).transpose(2, 0, 1)
        dw_out = total("blk,bld->kd", 3, 1).reshape(heads, head_dim, width)
        dw_down = total("blf,bld->fd", 2, 1)
        dw_gate = total("bld,blf->df", 0, 4)
        dw_up = total("bld,blf->df", 0, 5)

        y_parts, dx_parts = [], []
        gain_sum = 0.0
        for c in range(CHUNKS):
            residual, x_hat, inv_std = normalize(xs[c])
            y_parts.append((residual + ys[c].astype(F32)).astype(BF))
            dh = dhs[c].astype(F32)
            gain_sum += jnp.sum(dh * x_hat, axis=(0, 1))
            grad_hat = dh * ln_gain
            dx = inv_std * (grad_hat - jnp.mean(grad_hat, axis=-1, keepdims=True) - x_hat * jnp.mean(grad_hat * x_hat, axis=-1, keepdims=True)) + dys[c].astype(F32)
            dx_parts.append(dx.astype(BF))
        return (
            jnp.concatenate(y_parts, axis=0),
            jnp.concatenate(dx_parts, axis=0),
            lax.psum(gain_sum, "tp"),
            dw_query.astype(BF),
            dw_kv[:head_dim].T.astype(BF),
            dw_kv[head_dim:].T.astype(BF),
            dw_out.astype(BF),
            dw_gate.astype(BF),
            dw_up.astype(BF),
            dw_down.astype(BF),
        )

    act_spec = P(None, "tp", None)
    weight_specs = (P(), P(None, "tp", None), P(), P(), P("tp", None, None), P(None, "tp"), P(None, "tp"), P("tp", None))
    return jax.shard_map(layer_shard, mesh=mesh, in_specs=(act_spec, act_spec) + weight_specs, out_specs=(act_spec, act_spec) + weight_specs, check_vma=False)
```

```python
import functools

import jax
import jax.numpy as jnp
from jax import lax
from jax.experimental import pallas as pl
from jax.experimental.pallas import tpu as pltpu
from jax.sharding import PartitionSpec as P

LN_EPS = 1e-6
ROPE_BASE = 10000.0
BF = jnp.bfloat16
F32 = jnp.float32
VMEM_LIMIT = 67_043_328
NT_DIMS = (((1,), (1,)), ((), ()))


def rope_tables(seq_len, head_dim):
    half_dim = head_dim // 2
    inv_freq = ROPE_BASE ** (-jnp.arange(half_dim, dtype=F32) * 2.0 / head_dim)
    angles = jnp.arange(seq_len, dtype=F32)[:, None] * inv_freq[None, :]
    return jnp.cos(angles).T, jnp.sin(angles).T


def rotate(values, cos_tab, sin_tab):
    half = values.shape[0] // 2
    first, second = values[:half], values[half:]
    return jnp.concatenate([first * cos_tab - second * sin_tab, second * cos_tab + first * sin_tab], axis=0)


def attn_scores(k, q_t, scale, heads):
    seq = k.shape[0]
    scores = jnp.dot(k, q_t, preferred_element_type=F32) * scale
    key_pos = lax.broadcasted_iota(jnp.int32, (seq, heads * seq), 0)
    query_pos = lax.rem(lax.broadcasted_iota(jnp.int32, (seq, heads * seq), 1), seq)
    return jnp.where(key_pos <= query_pos, scores, -1e30)


def attn_fwd_kernel(heads, scale, qkv_ref, cos_ref, sin_ref, o_ref, rot_ref, stat_ref):
    hd = 2 * cos_ref.shape[0]
    cos, sin = cos_ref[...], sin_ref[...]
    seq = cos.shape[1]
    for b in range(qkv_ref.shape[1]):
        all_t = qkv_ref[:, b].reshape(seq, -1).T
        k_t = rotate(all_t[heads * hd:(heads + 1) * hd], cos, sin)
        v_t = all_t[(heads + 1) * hd:].astype(BF)
        rot_ref[b, heads * hd:(heads + 1) * hd] = k_t.astype(BF)
        rot_ref[b, (heads + 1) * hd:] = v_t
        q_t = [rotate(all_t[n * hd:(n + 1) * hd], cos, sin).astype(BF) for n in range(heads)]
        for n in range(heads):
            rot_ref[b, n * hd:(n + 1) * hd] = q_t[n]
        scores = attn_scores(k_t.T.astype(BF), jnp.concatenate(q_t, axis=1), scale, heads)
        top = jnp.max(scores, axis=0, keepdims=True)
        expd = jnp.exp(scores - top)
        inv = 1.0 / jnp.sum(expd, axis=0, keepdims=True)
        stat_ref[b, 0:1] = top
        stat_ref[b, 1:2] = inv
        outs = jnp.dot(v_t, (expd * inv).astype(BF), preferred_element_type=F32)
        outs = jnp.concatenate([outs[:, n * seq:(n + 1) * seq] for n in range(heads)], axis=0)
        o_ref[:, b] = outs.T.astype(BF).reshape(o_ref.shape[0], -1, heads * hd)


def attn_bwd_kernel(heads, scale, rot_ref, do_ref, stat_ref, cos_ref, sin_ref, dqkv_ref):
    hd = 2 * cos_ref.shape[0]
    cos, sin = cos_ref[...], sin_ref[...]
    seq = cos.shape[1]
    for b in range(do_ref.shape[1]):
        k_t = rot_ref[b, heads * hd:(heads + 1) * hd]
        v_t = rot_ref[b, (heads + 1) * hd:]
        do_all = do_ref[:, b].reshape(seq, -1).astype(F32).T.astype(BF)
        q_t = jnp.concatenate([rot_ref[b, n * hd:(n + 1) * hd] for n in range(heads)], axis=1)
        do_t = jnp.concatenate([do_all[n * hd:(n + 1) * hd] for n in range(heads)], axis=1)
        scores = attn_scores(k_t.astype(F32).T.astype(BF), q_t, scale, heads)
        probs = jnp.exp(scores - stat_ref[b, 0:1]) * stat_ref[b, 1:2]
        dprobs = jnp.dot(v_t.astype(F32).T.astype(BF), do_t, preferred_element_type=F32)
        row_dot = jnp.sum(probs * dprobs, axis=0, keepdims=True)
        dscores = (probs * (dprobs - row_dot) * scale).astype(BF)
        dq_t = jnp.dot(k_t, dscores, preferred_element_type=F32)
        grads = [rotate(dq_t[:, n * seq:(n + 1) * seq], cos, -sin) for n in range(heads)]
        dk_t = lax.dot_general(q_t, dscores, NT_DIMS, preferred_element_type=F32)
        dv_t = lax.dot_general(do_t, probs.astype(BF), NT_DIMS, preferred_element_type=F32)
        grads += [rotate(dk_t, cos, -sin), dv_t]
        dqkv_ref[:, b] = jnp.concatenate(grads, axis=0).T.astype(BF).reshape(dqkv_ref.shape[0], -1, dqkv_ref.shape[-1])


PER_STEP = 2


def attn_specs(devs, local):
    tokens = lambda c: pl.BlockSpec((devs, PER_STEP, local, c), lambda b: (0, b, 0, 0))
    block = lambda r, c: pl.BlockSpec((PER_STEP, r, c), lambda b: (b, 0, 0))
    return tokens, block


def attn_fwd(qkv, cos, sin, heads):
    devs, batch, local, rows = qkv.shape
    seq = devs * local
    hd = rows // (heads + 2)
    tokens, block = attn_specs(devs, local)
    table = pl.BlockSpec(cos.shape, lambda b: (0, 0))
    return pl.pallas_call(
        functools.partial(attn_fwd_kernel, heads, hd ** -0.5),
        grid=(batch // PER_STEP,),
        out_shape=(
            jax.ShapeDtypeStruct((devs, batch, local, heads * hd), BF),
            jax.ShapeDtypeStruct((batch, rows, seq), BF),
            jax.ShapeDtypeStruct((batch, 2, heads * seq), F32),
        ),
        in_specs=[tokens(rows), table, table],
        out_specs=(tokens(heads * hd), block(rows, seq), block(2, heads * seq)),
        compiler_params=pltpu.CompilerParams(vmem_limit_bytes=VMEM_LIMIT),
        cost_estimate=pl.CostEstimate(flops=batch * 10_000_000_00, bytes_accessed=batch * rows * seq * 8, transcendentals=0),
        name="attn_fwd",
    )(qkv, cos, sin)


def attn_bwd(rot, grad_heads, stat, cos, sin, heads):
    batch, rows, seq = rot.shape
    devs, _, local, _ = grad_heads.shape
    hd = rows // (heads + 2)
    tokens, block = attn_specs(devs, local)
    table = pl.BlockSpec(cos.shape, lambda b: (0, 0))
    return pl.pallas_call(
        functools.partial(attn_bwd_kernel, heads, hd ** -0.5),
        grid=(batch // PER_STEP,),
        out_shape=jax.ShapeDtypeStruct((devs, batch, local, rows), BF),
        in_specs=[block(rows, seq), tokens(heads * hd), block(2, heads * seq), table, table],
        out_specs=tokens(rows),
        compiler_params=pltpu.CompilerParams(vmem_limit_bytes=VMEM_LIMIT),
        cost_estimate=pl.CostEstimate(flops=batch * 20_000_000_00, bytes_accessed=batch * rows * seq * 6, transcendentals=0),
        name="attn_bwd",
    )(rot, grad_heads, stat, cos, sin)


UNIT_PIECES = (
    [[(0, g) for g in range(4)], [(1, g) for g in range(4)]]
    + [[(2, g), (3, g), (4, g), (5, g)] for g in range(4)]
    + [[(6, g), (7, g), (6, g + 2), (7, g + 2)] for g in range(2)]
)
SLOT = {piece: (u, p) for u, unit in enumerate(UNIT_PIECES) for p, piece in enumerate(unit)}
FORWARDS = (
    [((0, g), to) for g in range(4) for to in (2, 4, 1)]
    + [((2, g), 1) for g in range(4)] + [((4, g), 1) for g in range(4)] + [((6, g), 1) for g in range(4)]
    + [((4, g), 2) for g in (0, 1)] + [((2, g), 4) for g in (2, 3)]
)
SEND_INDEX = {f: i for i, f in enumerate(FORWARDS)}


def device_at(rel):
    me = lax.axis_index("tp")
    bits = [lax.rem(me, 2), lax.rem(me // 2, 2), me // 4]
    return sum((1 - bit if (rel >> k) & 1 else bit) * (1 << k) for k, bit in enumerate(bits))


class Gather:
    def __init__(self, buf, send_sem, recv_sem):
        self.buf, self.send_sem, self.recv_sem = buf, send_sem, recv_sem

    def copy(self, piece, to):
        src = SLOT[piece]
        dst = SLOT[(piece[0] ^ to, piece[1])]
        return pltpu.make_async_remote_copy(
            src_ref=self.buf.at[src], dst_ref=self.buf.at[dst],
            send_sem=self.send_sem.at[SEND_INDEX[(piece, to)]], recv_sem=self.recv_sem.at[dst],
            device_id=(device_at(to),), device_id_type=pl.DeviceIdType.MESH)

    def start(self, piece, to):
        self.copy(piece, to).start()

    def arrived(self, piece):
        rel, g = piece
        via = 1 if rel & 1 else (rel if rel != 6 else (2 if g < 2 else 4))
        self.copy((rel ^ via, g), via).wait_recv()

    def greet(self):
        barrier = pltpu.get_barrier_semaphore()
        for rel in (1, 2, 4):
            pl.semaphore_signal(barrier, inc=1, device_id=(device_at(rel),), device_id_type=pl.DeviceIdType.MESH)
        pl.semaphore_wait(barrier, 3)

    def pull(self, g):
        self.arrived((2, g))
        self.arrived((4, g))
        self.start((2, g), 1)
        self.start((4, g), 1)
        if g < 2:
            self.start((4, g), 2)
        else:
            self.start((2, g), 4)

    def pull_far(self, g):
        for k in (g, g + 2):
            self.arrived((6, k))
            self.start((6, k), 1)

    def finish(self):
        for piece, to in FORWARDS:
            self.copy(piece, to).wait_send()


def gate_up_kernel(tile, h_loc, w_gate, w_up, w_q, w_k, w_v, h_all, z_all, fa_all, fb_all, qkv_all, w_join,
                   hbuf, wg, wu, wq, z_st, fa_st, fb_st, qkv_st, send_sem, recv_sem, load_sem, w_sem, keep_sem, out_sem):
    step = pl.program_id(0)
    gather = Gather(hbuf, send_sem, recv_sem)
    width = wg.shape[1]
    tiles = width // tile

    def load(g):
        return pltpu.make_async_copy(h_loc.at[pl.ds(4 * g, 4)], hbuf.at[0, g], load_sem.at[g])

    def load_w(k, j):
        cols = pl.ds(j * tile, tile)
        src, dst = ((w_gate, wg), (w_up, wu))[k]
        return pltpu.make_async_copy(src.at[:, cols], dst.at[:, cols], w_sem.at[k, j])

    qrows, krows = w_q.shape[0], w_k.shape[0]
    load_q = [
        pltpu.make_async_copy(w_q, wq.at[pl.ds(0, qrows)], w_sem.at[2, 0]),
        pltpu.make_async_copy(w_k, wq.at[pl.ds(qrows, krows)], w_sem.at[2, 1]),
        pltpu.make_async_copy(w_v, wq.at[pl.ds(qrows + krows, krows)], w_sem.at[2, 2]),
    ]
    join = pltpu.make_async_copy(wq, w_join, w_sem.at[2, 3])

    def keep(u, p):
        rel, g = UNIT_PIECES[u][p]
        return pltpu.make_async_copy(hbuf.at[u, p], h_all.at[device_at(rel), pl.ds(4 * g, 4)], keep_sem.at[u, p])

    outs = ((z_st, z_all), (fa_st, fa_all), (fb_st, fb_all), (qkv_st, qkv_all))

    def put(u, k, p):
        rel, g = UNIT_PIECES[u][p]
        st, full = outs[k]
        return pltpu.make_async_copy(st.at[u % 2, p], full.at[device_at(rel), pl.ds(4 * g, 4)], out_sem.at[u % 2, k, p])

    def each(fn):
        for k in range(4):
            for p in range(4):
                fn(k, p)

    @pl.when(step == 0)
    def _():
        for g in range(4):
            load(g).start()
        for j in range(tiles):
            load_w(0, j).start()
            load_w(1, j).start()
        for c in load_q:
            c.start()
        gather.greet()
        for g in range(4):
            load(g).wait()
            for to in (2, 4, 1):
                gather.start((0, g), to)
            keep(0, g).start()

    @pl.when(step == 2)
    def _():
        for g in range(4):
            gather.arrived((1, g))
            keep(1, g).start()

    for q in range(4):
        @pl.when(step == 3 + 2 * q)
        def _():
            gather.pull(q)

        @pl.when(step == 4 + 2 * q)
        def _():
            gather.arrived((3, q))
            gather.arrived((5, q))
            for p in range(4):
                keep(2 + q, p).start()

    for g in range(2):
        @pl.when(step == 11 + 2 * g)
        def _():
            gather.pull_far(g)

        @pl.when(step == 12 + 2 * g)
        def _():
            gather.arrived((7, g))
            gather.arrived((7, g + 2))
            for p in range(4):
                keep(6 + g, p).start()

    for u in range(2, 8):
        @pl.when(step == 2 * u)
        def _():
            each(lambda k, p: put(u - 2, k, p).wait())

    unit = step // 2
    slot = lax.rem(unit, 2)

    def rows_of(ref):
        x = ref[unit]
        return x.reshape(-1, x.shape[-1])

    def gate_up(j):
        @pl.when(step == 0 if j < 3 else step == 1)
        def _():
            load_w(0, j).wait()
            load_w(1, j).wait()
        cols = pl.ds(j * tile, tile)
        gate = jnp.dot(rows_of(hbuf), wg[:, cols], preferred_element_type=F32)
        up = jnp.dot(rows_of(hbuf), wu[:, cols], preferred_element_type=F32)
        sig = jax.nn.sigmoid(gate)
        act = gate * sig
        shape = z_st.shape[1:-1] + (tile,)
        z_st[slot, :, :, :, cols] = (act * up).astype(BF).reshape(shape)
        fa_st[slot, :, :, :, cols] = (up * sig * (1.0 + gate * (1.0 - sig))).reshape(shape)
        fb_st[slot, :, :, :, cols] = act.reshape(shape)

    @pl.when(lax.rem(step, 2) == 0)
    def _():
        for j in range(3):
            gate_up(j)

    @pl.when(lax.rem(step, 2) == 1)
    def _():
        for j in range(3, tiles):
            gate_up(j)

        @pl.when(step == 1)
        def _():
            for c in load_q:
                c.wait()
            join.start()
        qkv = lax.dot_general(rows_of(hbuf), wq[...], NT_DIMS, preferred_element_type=F32)
        qkv_st[slot] = qkv.reshape(qkv_st.shape[1:])

    for u in range(8):
        @pl.when(step == 2 * u + 1)
        def _():
            each(lambda k, p: put(u, k, p).start())

    @pl.when(step == 15)
    def _():
        each(lambda k, p: put(6, k, p).wait())
        each(lambda k, p: put(7, k, p).wait())
        for u in range(8):
            for p in range(4):
                keep(u, p).wait()
        join.wait()
        gather.finish()


def gate_up_gather(h_loc, w_gate, w_up, w_q, w_k, w_v, tile=256):
    batch, local, width = h_loc.shape
    ffn, cols = w_gate.shape[1], w_q.shape[0] + w_k.shape[0] + w_v.shape[0]
    devs, quarter = 8, batch // 4
    tokens = devs * batch * local
    full = lambda c, t: jax.ShapeDtypeStruct((devs, batch, local, c), t)
    stage = lambda c, t: pltpu.VMEM((2, 4, quarter, local, c), t)
    return pl.pallas_call(
        functools.partial(gate_up_kernel, tile),
        grid=(16,),
        out_shape=(full(width, BF), full(ffn, BF), full(ffn, F32), full(ffn, F32), full(cols, F32), jax.ShapeDtypeStruct((cols, width), BF)),
        in_specs=[pl.BlockSpec(memory_space=pl.ANY)] * 6,
        out_specs=(pl.BlockSpec(memory_space=pl.ANY),) * 6,
        scratch_shapes=[
            pltpu.VMEM((8, 4, quarter, local, width), BF),
            pltpu.VMEM(w_gate.shape, BF), pltpu.VMEM(w_up.shape, BF), pltpu.VMEM((cols, width), BF),
            stage(ffn, BF), stage(ffn, F32), stage(ffn, F32), stage(cols, F32),
            pltpu.SemaphoreType.DMA((len(FORWARDS),)),
            pltpu.SemaphoreType.DMA((8, 4)),
            pltpu.SemaphoreType.DMA((4,)),
            pltpu.SemaphoreType.DMA((3, ffn // tile)),
            pltpu.SemaphoreType.DMA((8, 4)),
            pltpu.SemaphoreType.DMA((2, 4, 4)),
        ],
        compiler_params=pltpu.CompilerParams(collective_id=3, has_side_effects=True, vmem_limit_bytes=VMEM_LIMIT),
        cost_estimate=pl.CostEstimate(flops=2 * tokens * width * (2 * ffn + cols), bytes_accessed=tokens * (2 * width + 10 * ffn + 4 * cols), transcendentals=0),
        name="gate_up_gather",
    )(h_loc, w_gate, w_up, w_q, w_k, w_v)


class SmallSum:
    def __init__(self, part, out, pair_in, chip_sum, far_in, full, send_sem, recv_sem):
        self.part, self.out, self.pair_in, self.chip_sum, self.far_in, self.full = part, out, pair_in, chip_sum, far_in, full
        self.send_sem, self.recv_sem = send_sem, recv_sem
        self.me = lax.axis_index("tp")
        self.core, self.chip = lax.rem(self.me, 2), self.me // 2

    def remote(self, src, dst, k, rel):
        return pltpu.make_async_remote_copy(
            src_ref=src, dst_ref=dst, send_sem=self.send_sem.at[k], recv_sem=self.recv_sem.at[k],
            device_id=(device_at(rel),), device_id_type=pl.DeviceIdType.MESH)

    def pair(self, j):
        return self.remote(self.part.at[2 * j + 1 - self.core], self.pair_in.at[j], j, 1)

    def far(self, k):
        rel = 2 * (k + 1)
        return self.remote(self.chip_sum.at[device_at(rel) // 2], self.far_in.at[k], 4 + k, rel)

    def share(self, rel):
        return self.remote(self.full.at[self.me], self.full.at[self.me], 6 + rel, rel)

    def on_step(self, step, last):
        @pl.when(step == 0)
        def _():
            for j in range(4):
                self.pair(j).start()

        @pl.when(step == 2)
        def _():
            for j in range(4):
                self.pair(j).wait_recv()
                self.chip_sum[j] = self.part[2 * j + self.core] + self.pair_in[j]

        @pl.when(step == 3)
        def _():
            for k in range(3):
                self.far(k).start()

        @pl.when(step == last - 6)
        def _():
            total = self.chip_sum[self.chip]
            for k in range(3):
                self.far(k).wait_recv()
                total += self.far_in[k]
            self.full[self.me] = total.astype(BF)

        @pl.when(step == last - 5)
        def _():
            for rel in range(1, 8):
                self.share(rel).start()

        @pl.when(step == last)
        def _():
            for rel in range(1, 8):
                self.share(rel).wait_recv()
            self.out[...] = self.full[...]
            for j in range(4):
                self.pair(j).wait_send()
            for k in range(3):
                self.far(k).wait_send()
            for rel in range(1, 8):
                self.share(rel).wait_send()


def pair_matmul_kernel(num, trans, tiles, summed, *refs):
    a_hbm, b_refs = refs[:num], refs[num:2 * num]
    refs = refs[2 * num:]
    if summed:
        small_ref, out_ref, small_out = refs[:3]
        refs = refs[3:]
    else:
        out_ref, refs = refs[0], refs[1:]
    a_vmem = refs[:num]
    send_buf, recv_buf, a_sem, send_sem, recv_sem = refs[num:num + 5]
    step = pl.program_id(0)
    peers = range(1, 8) if summed else (1,)
    me = lax.axis_index("tp")
    core = lax.rem(me, 2)
    partner = me + 1 - 2 * core
    chips = a_vmem[0].shape[1]

    def load(half, which, chip):
        parity = 1 - core if half == 0 else core
        return pltpu.make_async_copy(a_hbm[which].at[chip, parity], a_vmem[which].at[half, chip], a_sem.at[half, which, chip])

    def exchange(tile):
        return pltpu.make_async_remote_copy(
            src_ref=send_buf.at[tile], dst_ref=recv_buf.at[tile], send_sem=send_sem.at[tile], recv_sem=recv_sem.at[tile],
            device_id=(partner,), device_id_type=pl.DeviceIdType.MESH)

    def product(half, rows):
        total = None
        for which in range(num):
            lhs = a_vmem[which][half, rows]
            lhs = lhs.reshape(-1, lhs.shape[-1])
            rhs = b_refs[which][...]
            term = lax.dot_general(lhs, rhs, NT_DIMS, preferred_element_type=F32) if trans[which] else jnp.dot(lhs, rhs, preferred_element_type=F32)
            total = term if total is None else total + term
        return total

    group = 1
    shape = (group,) + send_buf.shape[2:]

    @pl.when(step == 0)
    def _():
        for half in range(2):
            for which in range(num):
                for chip in range(chips):
                    load(half, which, chip).start()
        barrier = pltpu.get_barrier_semaphore()
        for rel in peers:
            pl.semaphore_signal(barrier, inc=1, device_id=(device_at(rel),), device_id_type=pl.DeviceIdType.MESH)
        pl.semaphore_wait(barrier, len(peers))
        for which in range(num):
            for chip in range(chips):
                load(0, which, chip).wait()

    if summed:
        SmallSum(small_ref, small_out, *refs[num + 5:]).on_step(step, 2 * tiles - 1)

    for tile in range(tiles):
        @pl.when(step == tile + 1)
        def _():
            exchange(tile).start()

    @pl.when(step == tiles)
    def _():
        for which in range(num):
            for chip in range(chips):
                load(1, which, chip).wait()

    for tile in range(tiles):
        @pl.when(step == tile + tiles)
        def _():
            exchange(tile).wait_recv()

    @pl.when(step < tiles)
    def _():
        @pl.loop(0, chips // group)
        def _(g):
            rows = pl.ds(g * group, group)
            send_buf[step, rows] = product(0, rows).astype(BF).reshape(shape)

    @pl.when(step >= tiles)
    def _():
        @pl.loop(0, chips // group)
        def _(g):
            rows = pl.ds(g * group, group)
            arrived = recv_buf[step - tiles, rows].reshape(-1, shape[-1])
            out_ref[rows] = (product(1, rows) + arrived.astype(F32)).astype(BF).reshape(shape)

    @pl.when(step == 2 * tiles - 1)
    def _():
        for tile in range(tiles):
            exchange(tile).wait_send()


def pair_matmul(lhs, rhs, trans, collective_id, name, tile=512, small=None):
    num = len(lhs)
    devs, batch, local = lhs[0].shape[:3]
    chips, seq = devs // 2, devs * local
    lhs = [a.reshape(chips, 2, batch, local, a.shape[-1]) for a in lhs]
    width = rhs[0].shape[0] if trans[0] else rhs[0].shape[1]
    tiles = width // tile
    in_specs = [pl.BlockSpec(memory_space=pl.ANY)] * num
    for b, t in zip(rhs, trans):
        if t:
            in_specs.append(pl.BlockSpec((tile, b.shape[1]), lambda i: (lax.rem(i, tiles), 0)))
        else:
            in_specs.append(pl.BlockSpec((b.shape[0], tile), lambda i: (0, lax.rem(i, tiles))))
    depth = sum(a.shape[-1] for a in lhs)
    out_shape = [jax.ShapeDtypeStruct((chips, batch, local, width), BF)]
    out_specs = [pl.BlockSpec((chips, batch, local, tile), lambda i: (0, 0, 0, lax.max(i - tiles, 0)))]
    scratch = [pltpu.VMEM((2, chips, batch, local, a.shape[-1]), BF) for a in lhs] + [
        pltpu.VMEM((tiles, chips, batch, local, tile), BF),
        pltpu.VMEM((tiles, chips, batch, local, tile), BF),
        pltpu.SemaphoreType.DMA((2, num, chips)),
        pltpu.SemaphoreType.DMA((tiles,)),
        pltpu.SemaphoreType.DMA((tiles,)),
    ]
    extra = []
    if small is not None:
        extra = [small]
        _, rows, cols = small.shape
        in_specs.append(pl.BlockSpec(small.shape, lambda i: (0, 0, 0), pipeline_mode=pl.Buffered(1)))
        out_shape.append(jax.ShapeDtypeStruct(small.shape, BF))
        out_specs.append(pl.BlockSpec(small.shape, lambda i: (0, 0, 0), pipeline_mode=pl.Buffered(1)))
        scratch += [pltpu.VMEM((4, rows, cols), F32), pltpu.VMEM((4, rows, cols), F32), pltpu.VMEM((3, rows, cols), F32),
                    pltpu.VMEM((8, rows, cols), BF), pltpu.SemaphoreType.DMA((14,)), pltpu.SemaphoreType.DMA((14,))]
    outs = pl.pallas_call(
        functools.partial(pair_matmul_kernel, num, trans, tiles, small is not None),
        grid=(2 * tiles,),
        out_shape=out_shape,
        in_specs=in_specs,
        out_specs=out_specs,
        scratch_shapes=scratch,
        compiler_params=pltpu.CompilerParams(collective_id=collective_id, has_side_effects=True, vmem_limit_bytes=VMEM_LIMIT),
        cost_estimate=pl.CostEstimate(flops=2 * batch * seq * width * depth, bytes_accessed=2 * depth * (batch * seq + width), transcendentals=0),
        name=name,
    )(*lhs, *rhs, *extra)
    return outs[0] if small is None else outs


ROWS = 16


def norm_kernel(x_ref, gain_ref, h_ref):
    per = x_ref.shape[1] // ROWS

    def rows_step(t, carry):
        where = (t // per, pl.ds(pl.multiple_of(lax.rem(t, per) * ROWS, ROWS), ROWS))
        x = x_ref[where].astype(F32)
        centered = x - jnp.mean(x, axis=-1, keepdims=True)
        inv_std = lax.rsqrt(jnp.mean(centered * centered, axis=-1, keepdims=True) + LN_EPS)
        h_ref[where] = (gain_ref[...] * (centered * inv_std)).astype(BF)
        return carry

    lax.fori_loop(0, x_ref.shape[0] * per, rows_step, 0, unroll=4)


def norm(x, gain, rows=8):
    batch, local, width = x.shape
    block = pl.BlockSpec((rows, local, width), lambda b: (b, 0, 0))
    return pl.pallas_call(
        norm_kernel,
        grid=(batch // rows,),
        out_shape=jax.ShapeDtypeStruct(x.shape, BF),
        in_specs=[block, pl.BlockSpec((width,), lambda b: (0,))],
        out_specs=block,
        compiler_params=pltpu.CompilerParams(vmem_limit_bytes=VMEM_LIMIT),
        name="norm",
    )(x, gain)


def finish_kernel(steps, x_ref, dh_ref, dy_ref, gain_ref, dx_ref, dgain_ref, acc, parts, send_sem, recv_sem):
    step = pl.program_id(0)
    me = lax.axis_index("tp")
    barrier = pltpu.get_barrier_semaphore()

    def share(rel):
        return pltpu.make_async_remote_copy(
            src_ref=parts.at[me], dst_ref=parts.at[me], send_sem=send_sem.at[rel], recv_sem=recv_sem.at[rel],
            device_id=(device_at(rel),), device_id_type=pl.DeviceIdType.MESH)

    @pl.when(step == 0)
    def _():
        acc[...] = jnp.zeros_like(acc)
        for rel in range(1, 8):
            pl.semaphore_signal(barrier, inc=1, device_id=(device_at(rel),), device_id_type=pl.DeviceIdType.MESH)

    per = x_ref.shape[1] // ROWS

    def rows_step(t, carry):
        where = (t // per, pl.ds(pl.multiple_of(lax.rem(t, per) * ROWS, ROWS), ROWS))
        x = x_ref[where].astype(F32)
        centered = x - jnp.mean(x, axis=-1, keepdims=True)
        inv_std = lax.rsqrt(jnp.mean(centered * centered, axis=-1, keepdims=True) + LN_EPS)
        x_hat = centered * inv_std
        dh = dh_ref[where].astype(F32)
        prod = dh * x_hat
        acc[...] += prod[:8] + prod[8:]
        grad_hat = dh * gain_ref[...]
        mean_hat = jnp.mean(grad_hat, axis=-1, keepdims=True)
        mean_dot = jnp.mean(grad_hat * x_hat, axis=-1, keepdims=True)
        dx_ref[where] = (inv_std * (grad_hat - mean_hat - x_hat * mean_dot) + dy_ref[where].astype(F32)).astype(BF)
        return carry

    lax.fori_loop(0, x_ref.shape[0] * per, rows_step, 0, unroll=4)

    @pl.when(step == steps - 1)
    def _():
        parts[me] = jnp.sum(acc[...], axis=0, keepdims=True)
        pl.semaphore_wait(barrier, 7)
        for rel in range(1, 8):
            share(rel).start()
        for rel in range(1, 8):
            share(rel).wait_recv()
        total = parts[0]
        for d in range(1, 8):
            total += parts[d]
        dgain_ref[...] = total
        for rel in range(1, 8):
            share(rel).wait_send()


def finish(x, dh, dy, gain, rows=8):
    batch, local, width = x.shape
    steps = batch // rows
    block = pl.BlockSpec((rows, local, width), lambda b: (b, 0, 0))
    return pl.pallas_call(
        functools.partial(finish_kernel, steps),
        grid=(steps,),
        out_shape=(jax.ShapeDtypeStruct(x.shape, BF), jax.ShapeDtypeStruct((1, width), F32)),
        in_specs=[block, block, block, pl.BlockSpec((width,), lambda b: (0,))],
        out_specs=(block, pl.BlockSpec((1, width), lambda b: (0, 0))),
        scratch_shapes=[pltpu.VMEM((8, width), F32), pltpu.VMEM((8, 1, width), F32), pltpu.SemaphoreType.DMA((8,)), pltpu.SemaphoreType.DMA((8,))],
        compiler_params=pltpu.CompilerParams(collective_id=4, has_side_effects=True, vmem_limit_bytes=VMEM_LIMIT),
        name="finish",
    )(x, dh, dy, gain)


def solution(mesh):
    group_size = mesh.shape["tp"]
    same_core = [[c + 2 * j for j in range(group_size // 2)] for c in range(2)]

    def layer_shard(x_loc, grad_y_loc, ln_gain, w_query, w_key, w_value, w_out, w_gate, w_up, w_down):
        head_dim = w_key.shape[1]
        heads = w_query.shape[1]
        width = x_loc.shape[2]
        seq_len = x_loc.shape[1] * group_size
        cos_tab, sin_tab = rope_tables(seq_len, head_dim)
        w_query_t = w_query.transpose(1, 2, 0).reshape(heads * head_dim, width)
        w_out_2d = w_out.reshape(heads * head_dim, width)

        normed_loc = norm(x_loc, ln_gain)
        normed, hidden, gate_factor, gate_act, qkv, w_qkv_t = gate_up_gather(normed_loc, w_gate, w_up, w_query_t, w_key.T, w_value.T)

        grad_in, _ = lax.optimization_barrier((grad_y_loc, qkv))
        grad = lax.all_gather(grad_in, "tp", axis=0, tiled=False)
        attn, rot, stat = attn_fwd(qkv, cos_tab, sin_tab, heads)
        branch = pair_matmul([hidden, attn], [w_down, w_out_2d], (False, False), 1, "branch_mm")
        y_sum = lax.psum_scatter(branch, "tp", scatter_dimension=0, tiled=False, axis_index_groups=same_core)

        grad_heads = jnp.einsum("abld,kd->ablk", grad, w_out_2d, preferred_element_type=F32).astype(BF)
        grad_hidden = jnp.einsum("abld,fd->ablf", grad, w_down, preferred_element_type=F32)
        grad_gate = (grad_hidden * gate_factor).astype(BF)
        grad_up = (grad_hidden * gate_act).astype(BF)
        dqkv = attn_bwd(rot, grad_heads, stat, cos_tab, sin_tab, heads)
        dw_qkv = jnp.einsum("zblk,zbld->kd", dqkv, normed, preferred_element_type=F32)
        kv_part = dw_qkv[heads * head_dim:].reshape(8, head_dim // 4, width)
        dh_part, dw_kv = pair_matmul([grad_gate, grad_up, dqkv], [w_gate, w_up, w_qkv_t], (True, True, False), 2, "dh_mm", tile=256, small=kv_part)
        dw_kv = dw_kv.reshape(2 * head_dim, width)
        dh_part, y_sum, normed, grad = lax.optimization_barrier((dh_part, y_sum, normed, grad))
        dh_sum = lax.psum_scatter(dh_part, "tp", scatter_dimension=0, tiled=False, axis_index_groups=same_core)

        total = lambda spec, a, b: jnp.einsum(spec, a, b, preferred_element_type=F32)
        dw_query = dw_qkv[:heads * head_dim].reshape(heads, head_dim, width).transpose(2, 0, 1)
        dw_out = total("zblk,zbld->kd", attn, grad).reshape(heads, head_dim, width)
        dw_down = total("zblf,zbld->fd", hidden, grad)
        dw_gate = total("zbld,zblf->df", normed, grad_gate)
        dw_up = total("zbld,zblf->df", normed, grad_up)

        dx, dgain = finish(x_loc, dh_sum, grad_y_loc, ln_gain)
        return (
            (x_loc.astype(F32) + y_sum.astype(F32)).astype(BF),
            dx,
            dgain.reshape(width),
            dw_query.astype(BF),
            dw_kv[:head_dim].T,
            dw_kv[head_dim:].T,
            dw_out.astype(BF),
            dw_gate.astype(BF),
            dw_up.astype(BF),
            dw_down.astype(BF),
        )

    act_spec = P(None, "tp", None)
    weight_specs = (P(), P(None, "tp", None), P(), P(), P("tp", None, None), P(None, "tp"), P(None, "tp"), P("tp", None))
    return jax.shard_map(layer_shard, mesh=mesh, in_specs=(act_spec, act_spec) + weight_specs, out_specs=(act_spec, act_spec) + weight_specs, check_vma=False)
```

```python
import functools

import jax
import jax.numpy as jnp
from jax import lax
from jax.experimental import pallas as pl
from jax.experimental.pallas import tpu as pltpu
from jax.sharding import PartitionSpec as P

LN_EPS = 1e-6
ROPE_BASE = 10000.0
BF = jnp.bfloat16
F32 = jnp.float32
VMEM_LIMIT = 67_043_328
PIECES = 4
DEVS = 8
SLOTS = 2
PEERS = range(1, DEVS)
NT_DIMS = (((1,), (1,)), ((), ()))


def row_mean(values):
    return jnp.mean(values, axis=-1, keepdims=True)


def rope_tables(seq_len, head_dim):
    half_dim = head_dim // SLOTS
    inv_freq = ROPE_BASE ** (-jnp.arange(half_dim, dtype=F32) * 2.0 / head_dim)
    angles = jnp.arange(seq_len, dtype=F32)[:, None] * inv_freq[None, :]
    return jnp.cos(angles).T, jnp.sin(angles).T


def rotate(values, cos_tab, sin_tab):
    half = values.shape[0] // SLOTS
    first, second = values[:half], values[half:]
    return jnp.concatenate([first * cos_tab - second * sin_tab, second * cos_tab + first * sin_tab], axis=0)


def attn_scores(k, q_t, scale, heads):
    seq = k.shape[0]
    scores = jnp.dot(k, q_t, preferred_element_type=F32) * scale
    key_pos = lax.broadcasted_iota(jnp.int32, (seq, heads * seq), 0)
    query_pos = lax.rem(lax.broadcasted_iota(jnp.int32, (seq, heads * seq), 1), seq)
    return jnp.where(key_pos <= query_pos, scores, -1e30)


def attn_fwd_kernel(heads, scale, qkv_ref, cos_ref, sin_ref, o_ref, rot_ref, stat_ref):
    hd = 2 * cos_ref.shape[0]
    cos, sin = cos_ref[...], sin_ref[...]
    seq = cos.shape[1]
    for b in range(qkv_ref.shape[1]):
        all_t = qkv_ref[:, b].reshape(seq, -1).T
        k_t = rotate(all_t[heads * hd:(heads + 1) * hd], cos, sin)
        v_t = all_t[(heads + 1) * hd:].astype(BF)
        rot_ref[b, heads * hd:(heads + 1) * hd] = k_t.astype(BF)
        rot_ref[b, (heads + 1) * hd:] = v_t
        q_t = [rotate(all_t[n * hd:(n + 1) * hd], cos, sin).astype(BF) for n in range(heads)]
        for n in range(heads):
            rot_ref[b, n * hd:(n + 1) * hd] = q_t[n]
        scores = attn_scores(k_t.T.astype(BF), jnp.concatenate(q_t, axis=1), scale, heads)
        top = jnp.max(scores, axis=0, keepdims=True)
        expd = jnp.exp(scores - top)
        inv = 1.0 / jnp.sum(expd, axis=0, keepdims=True)
        stat_ref[b, 0:1] = top
        stat_ref[b, 1:2] = inv
        outs = jnp.dot(v_t, (expd * inv).astype(BF), preferred_element_type=F32)
        outs = jnp.concatenate([outs[:, n * seq:(n + 1) * seq] for n in range(heads)], axis=0)
        o_ref[:, b] = outs.T.astype(BF).reshape(o_ref.shape[0], -1, heads * hd)


def attn_bwd_kernel(heads, scale, rot_ref, do_ref, stat_ref, cos_ref, sin_ref, dqkv_ref):
    hd = 2 * cos_ref.shape[0]
    cos, sin = cos_ref[...], sin_ref[...]
    seq = cos.shape[1]
    for b in range(do_ref.shape[1]):
        k_t = rot_ref[b, heads * hd:(heads + 1) * hd]
        v_t = rot_ref[b, (heads + 1) * hd:]
        do_all = do_ref[:, b].reshape(seq, -1).astype(F32).T.astype(BF)
        q_t = jnp.concatenate([rot_ref[b, n * hd:(n + 1) * hd] for n in range(heads)], axis=1)
        do_t = jnp.concatenate([do_all[n * hd:(n + 1) * hd] for n in range(heads)], axis=1)
        scores = attn_scores(k_t.astype(F32).T.astype(BF), q_t, scale, heads)
        probs = jnp.exp(scores - stat_ref[b, 0:1]) * stat_ref[b, 1:2]
        dprobs = jnp.dot(v_t.astype(F32).T.astype(BF), do_t, preferred_element_type=F32)
        row_dot = jnp.sum(probs * dprobs, axis=0, keepdims=True)
        dscores = (probs * (dprobs - row_dot) * scale).astype(BF)
        dq_t = jnp.dot(k_t, dscores, preferred_element_type=F32)
        grads = [rotate(dq_t[:, n * seq:(n + 1) * seq], cos, -sin) for n in range(heads)]
        dk_t = lax.dot_general(q_t, dscores, NT_DIMS, preferred_element_type=F32)
        dv_t = lax.dot_general(do_t, probs.astype(BF), NT_DIMS, preferred_element_type=F32)
        grads += [rotate(dk_t, cos, -sin), dv_t]
        dqkv_ref[:, b] = jnp.concatenate(grads, axis=0).T.astype(BF).reshape(dqkv_ref.shape[0], -1, dqkv_ref.shape[-1])


PER_STEP = PIECES


def attn_specs(devs, local):
    tokens = lambda c: pl.BlockSpec((devs, PER_STEP, local, c), lambda b: (0, b, 0, 0))
    block = lambda r, c: pl.BlockSpec((PER_STEP, r, c), lambda b: (b, 0, 0))
    return tokens, block


def attn_fwd(qkv, cos, sin, heads):
    devs, batch, local, rows = qkv.shape
    seq = devs * local
    hd = rows // (heads + 2)
    tokens, block = attn_specs(devs, local)
    table = pl.BlockSpec(cos.shape, lambda b: (0, 0))
    return pl.pallas_call(
        functools.partial(attn_fwd_kernel, heads, hd ** -0.5),
        grid=(batch // PER_STEP,),
        out_shape=(
            jax.ShapeDtypeStruct((devs, batch, local, heads * hd), BF),
            jax.ShapeDtypeStruct((batch, rows, seq), BF),
            jax.ShapeDtypeStruct((batch, 2, heads * seq), F32),
        ),
        in_specs=[tokens(rows), table, table],
        out_specs=(tokens(heads * hd), block(rows, seq), block(2, heads * seq)),
        compiler_params=pltpu.CompilerParams(vmem_limit_bytes=VMEM_LIMIT),
        cost_estimate=pl.CostEstimate(flops=batch * 10_000_000_00, bytes_accessed=batch * rows * seq * DEVS, transcendentals=0),
        name="attn_fwd",
    )(qkv, cos, sin)


def attn_bwd(rot, grad_heads, stat, cos, sin, heads):
    batch, rows, seq = rot.shape
    devs, _, local, _ = grad_heads.shape
    hd = rows // (heads + 2)
    tokens, block = attn_specs(devs, local)
    table = pl.BlockSpec(cos.shape, lambda b: (0, 0))
    return pl.pallas_call(
        functools.partial(attn_bwd_kernel, heads, hd ** -0.5),
        grid=(batch // PER_STEP,),
        out_shape=jax.ShapeDtypeStruct((devs, batch, local, rows), BF),
        in_specs=[block(rows, seq), tokens(heads * hd), block(2, heads * seq), table, table],
        out_specs=tokens(rows),
        compiler_params=pltpu.CompilerParams(vmem_limit_bytes=VMEM_LIMIT),
        cost_estimate=pl.CostEstimate(flops=batch * 20_000_000_00, bytes_accessed=batch * rows * seq * 6, transcendentals=0),
        name="attn_bwd",
    )(rot, grad_heads, stat, cos, sin)


UNIT_PIECES = (
    [[(0, g) for g in range(PIECES)], [(1, g) for g in range(PIECES)]]
    + [[(2, g), (3, g), (PIECES, g), (5, g)] for g in range(PIECES)]
    + [[(6, g), (7, g), (6, g + 2), (7, g + 2)] for g in range(2)]
)
SLOT = {piece: (u, p) for u, unit in enumerate(UNIT_PIECES) for p, piece in enumerate(unit)}
FORWARDS = (
    [((0, g), to) for g in range(PIECES) for to in (2, PIECES, 1)]
    + [((2, g), 1) for g in range(PIECES)] + [((PIECES, g), 1) for g in range(PIECES)] + [((6, g), 1) for g in range(PIECES)]
    + [((PIECES, g), 2) for g in (0, 1)] + [((2, g), PIECES) for g in (2, 3)]
)
SEND_INDEX = {f: i for i, f in enumerate(FORWARDS)}


def device_at(rel):
    me = lax.axis_index("tp")
    bits = [lax.rem(me, SLOTS), lax.rem(me // SLOTS, 2), me // PIECES]
    return sum((1 - bit if (rel >> k) & 1 else bit) * (1 << k) for k, bit in enumerate(bits))


class Gather:
    def __init__(self, buf, send_sem, recv_sem):
        self.buf, self.send_sem, self.recv_sem = buf, send_sem, recv_sem

    def copy(self, piece, to):
        src = SLOT[piece]
        dst = SLOT[(piece[0] ^ to, piece[1])]
        return pltpu.make_async_remote_copy(
            src_ref=self.buf.at[src], dst_ref=self.buf.at[dst],
            send_sem=self.send_sem.at[SEND_INDEX[(piece, to)]], recv_sem=self.recv_sem.at[dst],
            device_id=(device_at(to),), device_id_type=pl.DeviceIdType.MESH)

    def start(self, piece, to):
        self.copy(piece, to).start()

    def arrived(self, piece):
        rel, g = piece
        via = 1 if rel & 1 else (rel if rel != 6 else (2 if g < 2 else PIECES))
        self.copy((rel ^ via, g), via).wait_recv()

    def greet(self):
        barrier = pltpu.get_barrier_semaphore()
        for rel in (1, 2, PIECES):
            pl.semaphore_signal(barrier, inc=1, device_id=(device_at(rel),), device_id_type=pl.DeviceIdType.MESH)
        pl.semaphore_wait(barrier, 3)

    def pull(self, g):
        self.arrived((2, g))
        self.arrived((PIECES, g))
        self.start((2, g), 1)
        self.start((PIECES, g), 1)
        if g < 2:
            self.start((PIECES, g), 2)
        else:
            self.start((2, g), PIECES)

    def pull_far(self, g):
        for k in (g, g + 2):
            self.arrived((6, k))
            self.start((6, k), 1)

    def finish(self):
        for piece, to in FORWARDS:
            self.copy(piece, to).wait_send()


def gate_up_kernel(tile, h_loc, w_gate, w_up, w_q, w_k, w_v, h_all, z_all, fa_all, fb_all, qkv_all, w_join,
                   hbuf, wg, wu, wq, z_st, fa_st, fb_st, qkv_st, send_sem, recv_sem, load_sem, w_sem, keep_sem, out_sem):
    step = pl.program_id(0)
    gather = Gather(hbuf, send_sem, recv_sem)
    width = wg.shape[1]
    tiles = width // tile

    def load(g):
        return pltpu.make_async_copy(h_loc.at[pl.ds(PIECES * g, PIECES)], hbuf.at[0, g], load_sem.at[g])

    def load_w(k, j):
        cols = pl.ds(j * tile, tile)
        src, dst = ((w_gate, wg), (w_up, wu))[k]
        return pltpu.make_async_copy(src.at[:, cols], dst.at[:, cols], w_sem.at[k, j])

    qrows, krows = w_q.shape[0], w_k.shape[0]
    load_q = [
        pltpu.make_async_copy(w_q, wq.at[pl.ds(0, qrows)], w_sem.at[2, 0]),
        pltpu.make_async_copy(w_k, wq.at[pl.ds(qrows, krows)], w_sem.at[2, 1]),
        pltpu.make_async_copy(w_v, wq.at[pl.ds(qrows + krows, krows)], w_sem.at[2, 2]),
    ]
    join = pltpu.make_async_copy(wq, w_join, w_sem.at[2, 3])

    def keep(u, p):
        rel, g = UNIT_PIECES[u][p]
        return pltpu.make_async_copy(hbuf.at[u, p], h_all.at[device_at(rel), pl.ds(PIECES * g, PIECES)], keep_sem.at[u, p])

    outs = ((z_st, z_all), (fa_st, fa_all), (fb_st, fb_all), (qkv_st, qkv_all))

    def put(u, k, p):
        rel, g = UNIT_PIECES[u][p]
        st, full = outs[k]
        return pltpu.make_async_copy(st.at[u % SLOTS, p], full.at[device_at(rel), pl.ds(PIECES * g, PIECES)], out_sem.at[u % SLOTS, k, p])

    def each(fn):
        for k in range(PIECES):
            for p in range(PIECES):
                fn(k, p)

    @pl.when(step == 0)
    def _():
        for g in range(PIECES):
            load(g).start()
        for j in range(tiles):
            load_w(0, j).start()
            load_w(1, j).start()
        for c in load_q:
            c.start()
        gather.greet()
        for g in range(PIECES):
            load(g).wait()
            for to in (2, PIECES, 1):
                gather.start((0, g), to)
            keep(0, g).start()

    @pl.when(step == 2)
    def _():
        for g in range(PIECES):
            gather.arrived((1, g))
            keep(1, g).start()

    for q in range(PIECES):
        @pl.when(step == 3 + 2 * q)
        def _():
            gather.pull(q)

        @pl.when(step == PIECES + 2 * q)
        def _():
            gather.arrived((3, q))
            gather.arrived((5, q))
            for p in range(PIECES):
                keep(2 + q, p).start()

    for g in range(2):
        @pl.when(step == 11 + 2 * g)
        def _():
            gather.pull_far(g)

        @pl.when(step == 12 + 2 * g)
        def _():
            gather.arrived((7, g))
            gather.arrived((7, g + 2))
            for p in range(PIECES):
                keep(6 + g, p).start()

    for u in range(2, DEVS):
        @pl.when(step == 2 * u)
        def _():
            each(lambda k, p: put(u - 2, k, p).wait())

    unit = step // SLOTS
    slot = lax.rem(unit, SLOTS)

    def rows_of(ref):
        x = ref[unit]
        return x.reshape(-1, x.shape[-1])

    def gate_up(j):
        @pl.when(step == 0 if j < 3 else step == 1)
        def _():
            load_w(0, j).wait()
            load_w(1, j).wait()
        cols = pl.ds(j * tile, tile)
        gate = jnp.dot(rows_of(hbuf), wg[:, cols], preferred_element_type=F32)
        up = jnp.dot(rows_of(hbuf), wu[:, cols], preferred_element_type=F32)
        sig = jax.nn.sigmoid(gate)
        act = gate * sig
        shape = z_st.shape[1:-1] + (tile,)
        z_st[slot, :, :, :, cols] = (act * up).astype(BF).reshape(shape)
        fa_st[slot, :, :, :, cols] = (up * sig * (1.0 + gate * (1.0 - sig))).reshape(shape)
        fb_st[slot, :, :, :, cols] = act.reshape(shape)

    @pl.when(lax.rem(step, SLOTS) == 0)
    def _():
        for j in range(3):
            gate_up(j)

    @pl.when(lax.rem(step, SLOTS) == 1)
    def _():
        for j in range(3, tiles):
            gate_up(j)

        @pl.when(step == 1)
        def _():
            for c in load_q:
                c.wait()
            join.start()
        qkv = lax.dot_general(rows_of(hbuf), wq[...], NT_DIMS, preferred_element_type=F32)
        qkv_st[slot] = qkv.reshape(qkv_st.shape[1:])

    for u in range(DEVS):
        @pl.when(step == 2 * u + 1)
        def _():
            each(lambda k, p: put(u, k, p).start())

    @pl.when(step == 15)
    def _():
        each(lambda k, p: put(6, k, p).wait())
        each(lambda k, p: put(7, k, p).wait())
        for u in range(DEVS):
            for p in range(PIECES):
                keep(u, p).wait()
        join.wait()
        gather.finish()


def gate_up_gather(h_loc, w_gate, w_up, w_q, w_k, w_v, tile=256):
    batch, local, width = h_loc.shape
    ffn, cols = w_gate.shape[1], w_q.shape[0] + w_k.shape[0] + w_v.shape[0]
    devs, quarter = DEVS, batch // PIECES
    tokens = devs * batch * local
    full = lambda c, t: jax.ShapeDtypeStruct((devs, batch, local, c), t)
    stage = lambda c, t: pltpu.VMEM((2, PIECES, quarter, local, c), t)
    return pl.pallas_call(
        functools.partial(gate_up_kernel, tile),
        grid=(16,),
        out_shape=(full(width, BF), full(ffn, BF), full(ffn, F32), full(ffn, F32), full(cols, F32), jax.ShapeDtypeStruct((cols, width), BF)),
        in_specs=[pl.BlockSpec(memory_space=pl.ANY)] * 6,
        out_specs=(pl.BlockSpec(memory_space=pl.ANY),) * 6,
        scratch_shapes=[
            pltpu.VMEM((DEVS, PIECES, quarter, local, width), BF),
            pltpu.VMEM(w_gate.shape, BF), pltpu.VMEM(w_up.shape, BF), pltpu.VMEM((cols, width), BF),
            stage(ffn, BF), stage(ffn, F32), stage(ffn, F32), stage(cols, F32),
            pltpu.SemaphoreType.DMA((len(FORWARDS),)),
            pltpu.SemaphoreType.DMA((DEVS, PIECES)),
            pltpu.SemaphoreType.DMA((PIECES,)),
            pltpu.SemaphoreType.DMA((3, ffn // tile)),
            pltpu.SemaphoreType.DMA((DEVS, PIECES)),
            pltpu.SemaphoreType.DMA((2, PIECES, PIECES)),
        ],
        compiler_params=pltpu.CompilerParams(collective_id=3, has_side_effects=True, vmem_limit_bytes=VMEM_LIMIT),
        cost_estimate=pl.CostEstimate(flops=2 * tokens * width * (2 * ffn + cols), bytes_accessed=tokens * (2 * width + 10 * ffn + PIECES * cols), transcendentals=0),
        name="gate_up_gather",
    )(h_loc, w_gate, w_up, w_q, w_k, w_v)


PLAN = ["y", "d", "y", "d", "y", "d", "y", "d", "y", "y", "d", "y", "y", "d", "d", "d"]
Y_STEPS = [i for i, k in enumerate(PLAN) if k == "y"]
D_STEPS = [i for i, k in enumerate(PLAN) if k == "d"]
PULL_STEPS = {PIECES: 0, 6: 1, 9: 2, 12: 3}


def place(step, steps):
    return sum(jnp.where(step == at, i, 0) for i, at in enumerate(steps))


def one_of(step, steps):
    hit = step == steps[0]
    for at in steps[1:]:
        hit = hit | (step == at)
    return hit


def branch_gather_kernel(tile, ytile, dy_loc, z_all, o_all, fa_all, fb_all, w_down, w_out,
                         dy_all, branch, dgate_all, dup_all, do_all,
                         buf, wd, wo, z_st, o_st, fa_st, fb_st, dgate_st, dup_st, do_st, y_st, y_in,
                         send_sem, recv_sem, load_sem, w_sem, keep_sem, out_sem, f_sem, a_sem, ysend_sem, yrecv_sem, yout_sem):
    step = pl.program_id(0)
    gather = Gather(buf, send_sem, recv_sem)
    ffn = wd.shape[0]
    me = lax.axis_index("tp")
    core = lax.rem(me, SLOTS)

    def load(g):
        return pltpu.make_async_copy(dy_loc.at[pl.ds(PIECES * g, PIECES)], buf.at[0, g], load_sem.at[g])

    load_w = [pltpu.make_async_copy(w_down, wd, w_sem.at[0]), pltpu.make_async_copy(w_out, wo, w_sem.at[1])]

    def keep(u, p):
        rel, g = UNIT_PIECES[u][p]
        return pltpu.make_async_copy(buf.at[u, p], dy_all.at[device_at(rel), pl.ds(PIECES * g, PIECES)], keep_sem.at[u, p])

    def factors(u):
        for p, (rel, g) in enumerate(UNIT_PIECES[u]):
            where = (device_at(rel), pl.ds(PIECES * g, PIECES))
            yield pltpu.make_async_copy(fa_all.at[where], fa_st.at[p], f_sem.at[0, p])
            yield pltpu.make_async_copy(fb_all.at[where], fb_st.at[p], f_sem.at[1, p])

    def results(u):
        for p, (rel, g) in enumerate(UNIT_PIECES[u]):
            where = (device_at(rel), pl.ds(PIECES * g, PIECES))
            yield pltpu.make_async_copy(dgate_st.at[p], dgate_all.at[where], out_sem.at[0, p])
            yield pltpu.make_async_copy(dup_st.at[p], dup_all.at[where], out_sem.at[1, p])
            yield pltpu.make_async_copy(do_st.at[p], do_all.at[where], out_sem.at[2, p])

    def y_loads(i):
        dev = 2 * (i % PIECES) + (1 - core if i < PIECES else core)
        yield pltpu.make_async_copy(z_all.at[dev], z_st.at[i % SLOTS], a_sem.at[i % SLOTS, 0])
        yield pltpu.make_async_copy(o_all.at[dev], o_st.at[i % SLOTS], a_sem.at[i % SLOTS, 1])

    def y_exchange(i):
        return pltpu.make_async_remote_copy(
            src_ref=y_st.at[i % SLOTS], dst_ref=y_in.at[i], send_sem=ysend_sem.at[i], recv_sem=yrecv_sem.at[i],
            device_id=(device_at(1),), device_id_type=pl.DeviceIdType.MESH)

    def y_out(i):
        return pltpu.make_async_copy(y_st.at[i % SLOTS], branch.at[i - PIECES], yout_sem.at[i % SLOTS])

    def start(copies):
        for c in copies:
            c.start()

    def wait(copies):
        for c in copies:
            c.wait()

    @pl.when(step == 0)
    def _():
        for g in range(PIECES):
            load(g).start()
        start(y_loads(0))
        start(load_w)
        start(y_loads(1))
        start(factors(0))
        gather.greet()
        for g in range(PIECES):
            load(g).wait()
            for to in (2, PIECES, 1):
                gather.start((0, g), to)
            keep(0, g).start()
        wait(load_w)

    for i, at in enumerate(Y_STEPS):
        @pl.when(step == at + 1)
        def _():
            if i < PIECES:
                y_exchange(i).start()
            else:
                y_out(i).start()
            if i + 2 < DEVS:
                start(y_loads(i + 2))

    for u, at in enumerate(D_STEPS[:-1]):
        @pl.when(step == at + 1)
        def _():
            start(results(u))
            start(factors(u + 1))

    for at, q in PULL_STEPS.items():
        @pl.when(step == at)
        def _():
            gather.pull(q)

    for u, at in enumerate(D_STEPS):
        @pl.when(step == at)
        def _():
            if u == 1:
                for g in range(PIECES):
                    gather.arrived((1, g))
            elif 2 <= u < 6:
                gather.arrived((3, u - 2))
                gather.arrived((5, u - 2))
            elif u >= 6:
                gather.pull_far(u - 6)
                gather.arrived((7, u - 6))
                gather.arrived((7, u - PIECES))
            if u > 0:
                for p in range(PIECES):
                    keep(u, p).start()
                wait(results(u - 1))
            wait(factors(u))

    for i, at in enumerate(Y_STEPS):
        @pl.when(step == at)
        def _():
            wait(y_loads(i))
            if 2 <= i < 6:
                y_exchange(i - 2).wait_send()
            elif i >= 6:
                y_out(i - 2).wait()
            if i >= PIECES:
                y_exchange(i - PIECES).wait_recv()

    y_index = place(step, Y_STEPS)
    unit = place(step, D_STEPS)
    y_slot = lax.rem(y_index, SLOTS)
    shape = y_st.shape[1:-1] + (ytile,)

    def y_product(t):
        cols = pl.ds(pl.multiple_of(t * ytile, ytile), ytile)
        z = z_st[y_slot].reshape(-1, ffn)
        o = o_st[y_slot].reshape(-1, wo.shape[0])
        prod = jnp.dot(z, wd[:, cols], preferred_element_type=F32) + jnp.dot(o, wo[:, cols], preferred_element_type=F32)
        return cols, prod

    @pl.when(one_of(step, Y_STEPS[:PIECES]))
    def _():
        @pl.loop(0, wd.shape[1] // ytile)
        def _(t):
            cols, prod = y_product(t)
            y_st[y_slot, :, :, cols] = prod.astype(BF).reshape(shape)

    @pl.when(one_of(step, Y_STEPS[PIECES:]))
    def _():
        @pl.loop(0, wd.shape[1] // ytile)
        def _(t):
            cols, prod = y_product(t)
            other = y_in[y_index - PIECES, :, :, cols].reshape(prod.shape)
            y_st[y_slot, :, :, cols] = (prod + other.astype(F32)).astype(BF).reshape(shape)

    @pl.when(one_of(step, D_STEPS))
    def _():
        def rows():
            x = buf[unit]
            return x.reshape(-1, x.shape[-1])

        for j in range(ffn // tile):
            cols = slice(j * tile, (j + 1) * tile)
            dz = lax.dot_general(rows(), wd[cols], NT_DIMS, preferred_element_type=F32)
            dz = dz.reshape(fa_st.shape[:-1] + (tile,))
            dgate_st[:, :, :, cols] = (dz * fa_st[:, :, :, cols]).astype(BF)
            dup_st[:, :, :, cols] = (dz * fb_st[:, :, :, cols]).astype(BF)
        do = lax.dot_general(rows(), wo[...], NT_DIMS, preferred_element_type=F32)
        do_st[...] = do.astype(BF).reshape(do_st.shape)

    @pl.when(step == len(PLAN) - 1)
    def _():
        start(results(7))
        y_out(6).wait()
        y_out(7).wait()
        for u in range(DEVS):
            for p in range(PIECES):
                keep(u, p).wait()
        gather.finish()
        wait(results(7))


def branch_gather(dy_loc, z_all, o_all, fa_all, fb_all, w_down, w_out, tile=256, ytile=1280):
    batch, local, width = dy_loc.shape
    devs, ffn, qcols = z_all.shape[0], z_all.shape[-1], o_all.shape[-1]
    quarter = batch // PIECES
    tokens = devs * batch * local
    full = lambda c: jax.ShapeDtypeStruct((devs, batch, local, c), BF)
    stage = lambda c, t: pltpu.VMEM((PIECES, quarter, local, c), t)
    dma = lambda *n: pltpu.SemaphoreType.DMA(n)
    return pl.pallas_call(
        functools.partial(branch_gather_kernel, tile, ytile),
        grid=(len(PLAN),),
        out_shape=(full(width), jax.ShapeDtypeStruct((devs // SLOTS, batch, local, width), BF), full(ffn), full(ffn), full(qcols)),
        in_specs=[pl.BlockSpec(memory_space=pl.ANY)] * 7,
        out_specs=(pl.BlockSpec(memory_space=pl.ANY),) * 5,
        scratch_shapes=[
            pltpu.VMEM((DEVS, PIECES, quarter, local, width), BF),
            pltpu.VMEM(w_down.shape, BF), pltpu.VMEM(w_out.shape, BF),
            pltpu.VMEM((2, batch, local, ffn), BF), pltpu.VMEM((2, batch, local, qcols), BF),
            stage(ffn, F32), stage(ffn, F32), stage(ffn, BF), stage(ffn, BF), stage(qcols, BF),
            pltpu.VMEM((2, batch, local, width), BF), pltpu.VMEM((PIECES, batch, local, width), BF),
            dma(len(FORWARDS)), dma(DEVS, PIECES), dma(PIECES), dma(2), dma(DEVS, PIECES), dma(3, PIECES), dma(2, PIECES), dma(2, 2), dma(PIECES), dma(PIECES), dma(2),
        ],
        compiler_params=pltpu.CompilerParams(collective_id=1, has_side_effects=True, vmem_limit_bytes=VMEM_LIMIT),
        cost_estimate=pl.CostEstimate(flops=PIECES * tokens * width * (ffn + qcols), bytes_accessed=tokens * (6 * width + 14 * ffn + PIECES * qcols), transcendentals=0),
        name="branch_gather",
    )(dy_loc, z_all, o_all, fa_all, fb_all, w_down, w_out)


class SmallSum:
    def __init__(self, part, out, pair_in, chip_sum, far_in, full, send_sem, recv_sem):
        self.part, self.out, self.pair_in, self.chip_sum, self.far_in, self.full = part, out, pair_in, chip_sum, far_in, full
        self.send_sem, self.recv_sem = send_sem, recv_sem
        self.me = lax.axis_index("tp")
        self.core, self.chip = lax.rem(self.me, 2), self.me // SLOTS

    def remote(self, src, dst, k, rel):
        return pltpu.make_async_remote_copy(
            src_ref=src, dst_ref=dst, send_sem=self.send_sem.at[k], recv_sem=self.recv_sem.at[k],
            device_id=(device_at(rel),), device_id_type=pl.DeviceIdType.MESH)

    def pair(self, j):
        return self.remote(self.part.at[2 * j + 1 - self.core], self.pair_in.at[j], j, 1)

    def far(self, k):
        rel = 2 * (k + 1)
        return self.remote(self.chip_sum.at[device_at(rel) // SLOTS], self.far_in.at[k], PIECES + k, rel)

    def share(self, rel):
        return self.remote(self.full.at[self.me], self.full.at[self.me], 6 + rel, rel)

    def on_step(self, step, last):
        @pl.when(step == 0)
        def _():
            for j in range(PIECES):
                self.pair(j).start()

        @pl.when(step == 2)
        def _():
            for j in range(PIECES):
                self.pair(j).wait_recv()
                self.chip_sum[j] = self.part[2 * j + self.core] + self.pair_in[j]

        @pl.when(step == 3)
        def _():
            for k in range(3):
                self.far(k).start()

        @pl.when(step == last - 6)
        def _():
            total = self.chip_sum[self.chip]
            for k in range(3):
                self.far(k).wait_recv()
                total += self.far_in[k]
            self.full[self.me] = total.astype(BF)

        @pl.when(step == last - 5)
        def _():
            for rel in PEERS:
                self.share(rel).start()

        @pl.when(step == last)
        def _():
            for rel in PEERS:
                self.share(rel).wait_recv()
            self.out[...] = self.full[...]
            for j in range(PIECES):
                self.pair(j).wait_send()
            for k in range(3):
                self.far(k).wait_send()
            for rel in PEERS:
                self.share(rel).wait_send()


def pair_matmul_kernel(num, trans, tiles, summed, *refs):
    a_hbm, b_refs = refs[:num], refs[num:2 * num]
    refs = refs[2 * num:]
    if summed:
        small_ref, out_ref, small_out = refs[:3]
        refs = refs[3:]
    else:
        out_ref, refs = refs[0], refs[1:]
    a_vmem = refs[:num]
    send_buf, recv_buf, a_sem, send_sem, recv_sem = refs[num:num + 5]
    step = pl.program_id(0)
    peers = PEERS if summed else (1,)
    me = lax.axis_index("tp")
    core = lax.rem(me, SLOTS)
    partner = me + 1 - 2 * core
    chips = a_vmem[0].shape[1]

    def load(half, which, chip):
        parity = 1 - core if half == 0 else core
        return pltpu.make_async_copy(a_hbm[which].at[chip, parity], a_vmem[which].at[half, chip], a_sem.at[half, which, chip])

    def exchange(tile):
        return pltpu.make_async_remote_copy(
            src_ref=send_buf.at[tile], dst_ref=recv_buf.at[tile], send_sem=send_sem.at[tile], recv_sem=recv_sem.at[tile],
            device_id=(partner,), device_id_type=pl.DeviceIdType.MESH)

    def product(half, rows):
        total = None
        for which in range(num):
            lhs = a_vmem[which][half, rows]
            lhs = lhs.reshape(-1, lhs.shape[-1])
            rhs = b_refs[which][...]
            term = lax.dot_general(lhs, rhs, NT_DIMS, preferred_element_type=F32) if trans[which] else jnp.dot(lhs, rhs, preferred_element_type=F32)
            total = term if total is None else total + term
        return total

    group = PIECES
    shape = (group,) + send_buf.shape[2:]

    @pl.when(step == 0)
    def _():
        for half in range(2):
            for which in range(num):
                for chip in range(chips):
                    load(half, which, chip).start()
        barrier = pltpu.get_barrier_semaphore()
        for rel in peers:
            pl.semaphore_signal(barrier, inc=1, device_id=(device_at(rel),), device_id_type=pl.DeviceIdType.MESH)
        pl.semaphore_wait(barrier, len(peers))

    if summed:
        SmallSum(small_ref, small_out, *refs[num + 5:]).on_step(step, 2 * tiles - 1)

    for tile in range(tiles):
        @pl.when(step == tile + 1)
        def _():
            exchange(tile).start()

    @pl.when(step == tiles)
    def _():
        for which in range(num):
            for chip in range(chips):
                load(1, which, chip).wait()

    for tile in range(tiles):
        @pl.when(step == tile + tiles)
        def _():
            exchange(tile).wait_recv()

    @pl.when(step < tiles)
    def _():
        @pl.loop(0, chips // group)
        def _(g):
            @pl.when(step == 0)
            def _():
                for which in range(num):
                    for chip in range(group):
                        load(0, which, g * group + chip).wait()
            rows = pl.ds(g * group, group)
            send_buf[step, rows] = product(0, rows).astype(BF).reshape(shape)

    @pl.when(step >= tiles)
    def _():
        @pl.loop(0, chips // group)
        def _(g):
            rows = pl.ds(g * group, group)
            arrived = recv_buf[step - tiles, rows].reshape(-1, shape[-1])
            out_ref[rows] = (product(1, rows) + arrived.astype(F32)).astype(BF).reshape(shape)

    @pl.when(step == 2 * tiles - 1)
    def _():
        for tile in range(tiles):
            exchange(tile).wait_send()


def pair_matmul(lhs, rhs, trans, collective_id, name, tile=512, small=None):
    num = len(lhs)
    devs, batch, local = lhs[0].shape[:3]
    chips, seq = devs // SLOTS, devs * local
    lhs = [a.reshape(chips, 2, batch, local, a.shape[-1]) for a in lhs]
    width = rhs[0].shape[0] if trans[0] else rhs[0].shape[1]
    tiles = width // tile
    in_specs = [pl.BlockSpec(memory_space=pl.ANY)] * num
    for b, t in zip(rhs, trans):
        if t:
            in_specs.append(pl.BlockSpec((tile, b.shape[1]), lambda i: (lax.rem(i, tiles), 0)))
        else:
            in_specs.append(pl.BlockSpec((b.shape[0], tile), lambda i: (0, lax.rem(i, tiles))))
    depth = sum(a.shape[-1] for a in lhs)
    out_shape = [jax.ShapeDtypeStruct((chips, batch, local, width), BF)]
    out_specs = [pl.BlockSpec((chips, batch, local, tile), lambda i: (0, 0, 0, lax.max(i - tiles, 0)))]
    scratch = [pltpu.VMEM((2, chips, batch, local, a.shape[-1]), BF) for a in lhs] + [
        pltpu.VMEM((tiles, chips, batch, local, tile), BF),
        pltpu.VMEM((tiles, chips, batch, local, tile), BF),
        pltpu.SemaphoreType.DMA((2, num, chips)),
        pltpu.SemaphoreType.DMA((tiles,)),
        pltpu.SemaphoreType.DMA((tiles,)),
    ]
    extra = []
    if small is not None:
        extra = [small]
        _, rows, cols = small.shape
        in_specs.append(pl.BlockSpec(small.shape, lambda i: (0, 0, 0), pipeline_mode=pl.Buffered(1)))
        out_shape.append(jax.ShapeDtypeStruct(small.shape, BF))
        out_specs.append(pl.BlockSpec(small.shape, lambda i: (0, 0, 0), pipeline_mode=pl.Buffered(1)))
        scratch += [pltpu.VMEM((PIECES, rows, cols), F32), pltpu.VMEM((PIECES, rows, cols), F32), pltpu.VMEM((3, rows, cols), F32),
                    pltpu.VMEM((DEVS, rows, cols), BF), pltpu.SemaphoreType.DMA((14,)), pltpu.SemaphoreType.DMA((14,))]
    outs = pl.pallas_call(
        functools.partial(pair_matmul_kernel, num, trans, tiles, small is not None),
        grid=(2 * tiles,),
        out_shape=out_shape,
        in_specs=in_specs,
        out_specs=out_specs,
        scratch_shapes=scratch,
        compiler_params=pltpu.CompilerParams(collective_id=collective_id, has_side_effects=True, vmem_limit_bytes=VMEM_LIMIT),
        cost_estimate=pl.CostEstimate(flops=2 * batch * seq * width * depth, bytes_accessed=2 * depth * (batch * seq + width), transcendentals=0),
        name=name,
    )(*lhs, *rhs, *extra)
    return outs[0] if small is None else outs


ROWS = 16


def norm_kernel(x_ref, gain_ref, h_ref):
    per = x_ref.shape[1] // ROWS

    def rows_step(t, carry):
        where = (t // per, pl.ds(pl.multiple_of(lax.rem(t, per) * ROWS, ROWS), ROWS))
        x = x_ref[where].astype(F32)
        centered = x - row_mean(x)
        inv_std = lax.rsqrt(row_mean(centered * centered) + LN_EPS)
        h_ref[where] = (gain_ref[...] * (centered * inv_std)).astype(BF)
        return carry

    lax.fori_loop(0, x_ref.shape[0] * per, rows_step, 0, unroll=PIECES)


def norm(x, gain, rows=DEVS):
    batch, local, width = x.shape
    block = pl.BlockSpec((rows, local, width), lambda b: (b, 0, 0))
    return pl.pallas_call(
        norm_kernel,
        grid=(batch // rows,),
        out_shape=jax.ShapeDtypeStruct(x.shape, BF),
        in_specs=[block, pl.BlockSpec((width,), lambda b: (0,))],
        out_specs=block,
        compiler_params=pltpu.CompilerParams(vmem_limit_bytes=VMEM_LIMIT),
        name="norm",
    )(x, gain)


def finish_kernel(steps, x_ref, dh_ref, dy_ref, gain_ref, dx_ref, dgain_ref, acc, parts, send_sem, recv_sem):
    step = pl.program_id(0)
    me = lax.axis_index("tp")
    barrier = pltpu.get_barrier_semaphore()

    def share(rel):
        return pltpu.make_async_remote_copy(
            src_ref=parts.at[me], dst_ref=parts.at[me], send_sem=send_sem.at[rel], recv_sem=recv_sem.at[rel],
            device_id=(device_at(rel),), device_id_type=pl.DeviceIdType.MESH)

    @pl.when(step == 0)
    def _():
        acc[...] = jnp.zeros_like(acc)
        for rel in PEERS:
            pl.semaphore_signal(barrier, inc=1, device_id=(device_at(rel),), device_id_type=pl.DeviceIdType.MESH)

    per = x_ref.shape[1] // ROWS

    def rows_step(t, carry):
        where = (t // per, pl.ds(pl.multiple_of(lax.rem(t, per) * ROWS, ROWS), ROWS))
        x = x_ref[where].astype(F32)
        centered = x - row_mean(x)
        inv_std = lax.rsqrt(row_mean(centered * centered) + LN_EPS)
        x_hat = centered * inv_std
        dh = dh_ref[where].astype(F32)
        prod = dh * x_hat
        acc[...] += prod[:DEVS] + prod[DEVS:]
        grad_hat = dh * gain_ref[...]
        mean_hat = row_mean(grad_hat)
        mean_dot = row_mean(grad_hat * x_hat)
        dx_ref[where] = (inv_std * (grad_hat - mean_hat - x_hat * mean_dot) + dy_ref[where].astype(F32)).astype(BF)
        return carry

    lax.fori_loop(0, x_ref.shape[0] * per, rows_step, 0, unroll=PIECES)

    @pl.when(step == steps - 1)
    def _():
        parts[me] = jnp.sum(acc[...], axis=0, keepdims=True)
        pl.semaphore_wait(barrier, 7)
        for rel in PEERS:
            share(rel).start()
        for rel in PEERS:
            share(rel).wait_recv()
        total = parts[0]
        for d in PEERS:
            total += parts[d]
        dgain_ref[...] = total.reshape(-1)
        for rel in PEERS:
            share(rel).wait_send()


def finish(x, dh, dy, gain, rows=DEVS):
    batch, local, width = x.shape
    steps = batch // rows
    block = pl.BlockSpec((rows, local, width), lambda b: (b, 0, 0))
    return pl.pallas_call(
        functools.partial(finish_kernel, steps),
        grid=(steps,),
        out_shape=(jax.ShapeDtypeStruct(x.shape, BF), jax.ShapeDtypeStruct((width,), F32)),
        in_specs=[block, block, block, pl.BlockSpec((width,), lambda b: (0,))],
        out_specs=(block, pl.BlockSpec((width,), lambda b: (0,))),
        scratch_shapes=[pltpu.VMEM((DEVS, width), F32), pltpu.VMEM((DEVS, 1, width), F32), pltpu.SemaphoreType.DMA((DEVS,)), pltpu.SemaphoreType.DMA((DEVS,))],
        compiler_params=pltpu.CompilerParams(collective_id=PIECES, has_side_effects=True, vmem_limit_bytes=VMEM_LIMIT),
        name="finish",
    )(x, dh, dy, gain)


def solution(mesh):
    group_size = mesh.shape["tp"]
    same_core = [[c + 2 * j for j in range(group_size // SLOTS)] for c in range(2)]

    def layer_shard(x_loc, grad_y_loc, ln_gain, w_query, w_key, w_value, w_out, w_gate, w_up, w_down):
        head_dim = w_key.shape[1]
        heads = w_query.shape[1]
        width = x_loc.shape[2]
        seq_len = x_loc.shape[1] * group_size
        cos_tab, sin_tab = rope_tables(seq_len, head_dim)
        w_query_t = w_query.transpose(1, 2, 0).reshape(heads * head_dim, width)
        w_out_2d = w_out.reshape(heads * head_dim, width)

        normed_loc = norm(x_loc, ln_gain)
        normed, hidden, gate_factor, gate_act, qkv, w_qkv_t = gate_up_gather(normed_loc, w_gate, w_up, w_query_t, w_key.T, w_value.T)

        attn, rot, stat = attn_fwd(qkv, cos_tab, sin_tab, heads)
        grad, branch, grad_gate, grad_up, grad_heads = branch_gather(grad_y_loc, hidden, attn, gate_factor, gate_act, w_down, w_out_2d)
        y_sum = lax.psum_scatter(branch, "tp", scatter_dimension=0, tiled=False, axis_index_groups=same_core)

        dqkv = attn_bwd(rot, grad_heads, stat, cos_tab, sin_tab, heads)
        dw_qkv = jnp.einsum("zblk,zbld->kd", dqkv, normed, preferred_element_type=F32)
        kv_part = dw_qkv[heads * head_dim:].reshape(DEVS, head_dim // PIECES, width)
        dh_part, dw_kv = pair_matmul([grad_gate, grad_up, dqkv], [w_gate, w_up, w_qkv_t], (True, True, False), 2, "dh_mm", tile=256, small=kv_part)
        dw_kv = dw_kv.reshape(2 * head_dim, width)
        dh_part, y_sum, normed, grad = lax.optimization_barrier((dh_part, y_sum, normed, grad))
        dh_sum = lax.psum_scatter(dh_part, "tp", scatter_dimension=0, tiled=False, axis_index_groups=same_core)

        total = lambda spec, a, b: jnp.einsum(spec, a, b, preferred_element_type=F32)
        dw_query = dw_qkv[:heads * head_dim].reshape(heads, head_dim, width).transpose(2, 0, 1)
        dw_out = total("zblk,zbld->kd", attn, grad).reshape(heads, head_dim, width)
        dw_down = total("zblf,zbld->fd", hidden, grad)
        dw_gate = total("zbld,zblf->df", normed, grad_gate)
        dw_up = total("zbld,zblf->df", normed, grad_up)

        dx, dgain = finish(x_loc, dh_sum, grad_y_loc, ln_gain)
        return (
            (x_loc.astype(F32) + y_sum.astype(F32)).astype(BF),
            dx,
            dgain,
            dw_query.astype(BF),
            dw_kv[:head_dim].T,
            dw_kv[head_dim:].T,
            dw_out.astype(BF),
            dw_gate.astype(BF),
            dw_up.astype(BF),
            dw_down.astype(BF),
        )

    act_spec = P(None, "tp", None)
    weight_specs = (P(), P(None, "tp", None), P(), P(), P("tp", None, None), P(None, "tp"), P(None, "tp"), P("tp", None))
    return jax.shard_map(layer_shard, mesh=mesh, in_specs=(act_spec, act_spec) + weight_specs, out_specs=(act_spec, act_spec) + weight_specs, check_vma=False)
```

```python
import functools

import jax
import jax.numpy as jnp
from jax import lax
from jax.experimental import pallas as pl
from jax.experimental.pallas import tpu as pltpu
from jax.sharding import PartitionSpec as P

LN_EPS = 1e-6
ROPE_BASE = 10000.0
BF = jnp.bfloat16
F32 = jnp.float32
VMEM_LIMIT = 67_043_328
PIECES = 4
DEVS = 8
SLOTS = 2
PEERS = range(1, DEVS)
NT_DIMS = (((1,), (1,)), ((), ()))


def row_mean(values):
    return jnp.mean(values, axis=-1, keepdims=True)


def rope_tables(seq_len, head_dim):
    half_dim = head_dim // SLOTS
    inv_freq = ROPE_BASE ** (-jnp.arange(half_dim, dtype=F32) * 2.0 / head_dim)
    angles = jnp.arange(seq_len, dtype=F32)[:, None] * inv_freq[None, :]
    return jnp.cos(angles).T, jnp.sin(angles).T


def rotate(values, cos_tab, sin_tab):
    half = values.shape[0] // SLOTS
    first, second = values[:half], values[half:]
    return jnp.concatenate([first * cos_tab - second * sin_tab, second * cos_tab + first * sin_tab], axis=0)


def attn_scores(k, q_t, scale, heads):
    seq = k.shape[0]
    scores = jnp.dot(k, q_t, preferred_element_type=F32) * scale
    key_pos = lax.broadcasted_iota(jnp.int32, (seq, heads * seq), 0)
    query_pos = lax.rem(lax.broadcasted_iota(jnp.int32, (seq, heads * seq), 1), seq)
    return jnp.where(key_pos <= query_pos, scores, -1e30)


def attn_fwd_kernel(heads, scale, qkv_ref, cos_ref, sin_ref, o_ref, rot_ref, stat_ref):
    hd = 2 * cos_ref.shape[0]
    cos, sin = cos_ref[...], sin_ref[...]
    seq = cos.shape[1]
    for b in range(qkv_ref.shape[1]):
        all_t = qkv_ref[:, b].reshape(seq, -1).T
        k_t = rotate(all_t[heads * hd:(heads + 1) * hd], cos, sin)
        v_t = all_t[(heads + 1) * hd:].astype(BF)
        rot_ref[b, heads * hd:(heads + 1) * hd] = k_t.astype(BF)
        rot_ref[b, (heads + 1) * hd:] = v_t
        q_t = [rotate(all_t[n * hd:(n + 1) * hd], cos, sin).astype(BF) for n in range(heads)]
        for n in range(heads):
            rot_ref[b, n * hd:(n + 1) * hd] = q_t[n]
        scores = attn_scores(k_t.T.astype(BF), jnp.concatenate(q_t, axis=1), scale, heads)
        top = jnp.max(scores, axis=0, keepdims=True)
        expd = jnp.exp(scores - top)
        inv = 1.0 / jnp.sum(expd, axis=0, keepdims=True)
        stat_ref[b, 0:1] = top
        stat_ref[b, 1:2] = inv
        outs = jnp.dot(v_t, (expd * inv).astype(BF), preferred_element_type=F32)
        outs = jnp.concatenate([outs[:, n * seq:(n + 1) * seq] for n in range(heads)], axis=0)
        o_ref[:, b] = outs.T.astype(BF).reshape(o_ref.shape[0], -1, heads * hd)


def attn_bwd_kernel(heads, scale, rot_ref, do_ref, stat_ref, cos_ref, sin_ref, dqkv_ref):
    hd = 2 * cos_ref.shape[0]
    cos, sin = cos_ref[...], sin_ref[...]
    seq = cos.shape[1]
    for b in range(do_ref.shape[1]):
        k_t = rot_ref[b, heads * hd:(heads + 1) * hd]
        v_t = rot_ref[b, (heads + 1) * hd:]
        do_all = do_ref[:, b].reshape(seq, -1).astype(F32).T.astype(BF)
        q_t = jnp.concatenate([rot_ref[b, n * hd:(n + 1) * hd] for n in range(heads)], axis=1)
        do_t = jnp.concatenate([do_all[n * hd:(n + 1) * hd] for n in range(heads)], axis=1)
        scores = attn_scores(k_t.astype(F32).T.astype(BF), q_t, scale, heads)
        probs = jnp.exp(scores - stat_ref[b, 0:1]) * stat_ref[b, 1:2]
        dprobs = jnp.dot(v_t.astype(F32).T.astype(BF), do_t, preferred_element_type=F32)
        row_dot = jnp.sum(probs * dprobs, axis=0, keepdims=True)
        dscores = (probs * (dprobs - row_dot) * scale).astype(BF)
        dq_t = jnp.dot(k_t, dscores, preferred_element_type=F32)
        grads = [rotate(dq_t[:, n * seq:(n + 1) * seq], cos, -sin) for n in range(heads)]
        dk_t = lax.dot_general(q_t, dscores, NT_DIMS, preferred_element_type=F32)
        dv_t = lax.dot_general(do_t, probs.astype(BF), NT_DIMS, preferred_element_type=F32)
        grads += [rotate(dk_t, cos, -sin), dv_t]
        dqkv_ref[:, b] = jnp.concatenate(grads, axis=0).T.astype(BF).reshape(dqkv_ref.shape[0], -1, dqkv_ref.shape[-1])


PER_STEP = PIECES


def attn_specs(devs, local):
    tokens = lambda c: pl.BlockSpec((devs, PER_STEP, local, c), lambda b: (0, b, 0, 0))
    block = lambda r, c: pl.BlockSpec((PER_STEP, r, c), lambda b: (b, 0, 0))
    return tokens, block


def attn_fwd(qkv, cos, sin, heads):
    devs, batch, local, rows = qkv.shape
    seq = devs * local
    hd = rows // (heads + 2)
    tokens, block = attn_specs(devs, local)
    table = pl.BlockSpec(cos.shape, lambda b: (0, 0))
    return pl.pallas_call(
        functools.partial(attn_fwd_kernel, heads, hd ** -0.5),
        grid=(batch // PER_STEP,),
        out_shape=(
            jax.ShapeDtypeStruct((devs, batch, local, heads * hd), BF),
            jax.ShapeDtypeStruct((batch, rows, seq), BF),
            jax.ShapeDtypeStruct((batch, 2, heads * seq), F32),
        ),
        in_specs=[tokens(rows), table, table],
        out_specs=(tokens(heads * hd), block(rows, seq), block(2, heads * seq)),
        compiler_params=pltpu.CompilerParams(vmem_limit_bytes=VMEM_LIMIT),
        cost_estimate=pl.CostEstimate(flops=batch * 10_000_000_00, bytes_accessed=batch * rows * seq * DEVS, transcendentals=0),
        name="attn_fwd",
    )(qkv, cos, sin)


def attn_bwd(rot, grad_heads, stat, cos, sin, heads):
    batch, rows, seq = rot.shape
    devs, _, local, _ = grad_heads.shape
    hd = rows // (heads + 2)
    tokens, block = attn_specs(devs, local)
    table = pl.BlockSpec(cos.shape, lambda b: (0, 0))
    return pl.pallas_call(
        functools.partial(attn_bwd_kernel, heads, hd ** -0.5),
        grid=(batch // PER_STEP,),
        out_shape=jax.ShapeDtypeStruct((devs, batch, local, rows), BF),
        in_specs=[block(rows, seq), tokens(heads * hd), block(2, heads * seq), table, table],
        out_specs=tokens(rows),
        compiler_params=pltpu.CompilerParams(vmem_limit_bytes=VMEM_LIMIT),
        cost_estimate=pl.CostEstimate(flops=batch * 20_000_000_00, bytes_accessed=batch * rows * seq * 6, transcendentals=0),
        name="attn_bwd",
    )(rot, grad_heads, stat, cos, sin)


UNIT_PIECES = (
    [[(0, g) for g in range(PIECES)], [(1, g) for g in range(PIECES)]]
    + [[(2, g), (3, g), (PIECES, g), (5, g)] for g in range(PIECES)]
    + [[(6, g), (7, g), (6, g + 2), (7, g + 2)] for g in range(2)]
)
SLOT = {piece: (u, p) for u, unit in enumerate(UNIT_PIECES) for p, piece in enumerate(unit)}
FORWARDS = (
    [((0, g), to) for g in range(PIECES) for to in (2, PIECES, 1)]
    + [((2, g), 1) for g in range(PIECES)] + [((PIECES, g), 1) for g in range(PIECES)] + [((6, g), 1) for g in range(PIECES)]
    + [((PIECES, g), 2) for g in (0, 1)] + [((2, g), PIECES) for g in (2, 3)]
)
SEND_INDEX = {f: i for i, f in enumerate(FORWARDS)}


def device_at(rel):
    me = lax.axis_index("tp")
    bits = [lax.rem(me, SLOTS), lax.rem(me // SLOTS, 2), me // PIECES]
    return sum((1 - bit if (rel >> k) & 1 else bit) * (1 << k) for k, bit in enumerate(bits))


class Gather:
    def __init__(self, buf, send_sem, recv_sem):
        self.buf, self.send_sem, self.recv_sem = buf, send_sem, recv_sem

    def copy(self, piece, to):
        src = SLOT[piece]
        dst = SLOT[(piece[0] ^ to, piece[1])]
        return pltpu.make_async_remote_copy(
            src_ref=self.buf.at[src], dst_ref=self.buf.at[dst],
            send_sem=self.send_sem.at[SEND_INDEX[(piece, to)]], recv_sem=self.recv_sem.at[dst],
            device_id=(device_at(to),), device_id_type=pl.DeviceIdType.MESH)

    def start(self, piece, to):
        self.copy(piece, to).start()

    def arrived(self, piece):
        rel, g = piece
        via = 1 if rel & 1 else (rel if rel != 6 else (2 if g < 2 else PIECES))
        self.copy((rel ^ via, g), via).wait_recv()

    def greet(self):
        barrier = pltpu.get_barrier_semaphore()
        for rel in (1, 2, PIECES):
            pl.semaphore_signal(barrier, inc=1, device_id=(device_at(rel),), device_id_type=pl.DeviceIdType.MESH)
        pl.semaphore_wait(barrier, 3)

    def pull(self, g):
        self.arrived((2, g))
        self.arrived((PIECES, g))
        self.start((2, g), 1)
        self.start((PIECES, g), 1)
        if g < 2:
            self.start((PIECES, g), 2)
        else:
            self.start((2, g), PIECES)

    def pull_far(self, g):
        for k in (g, g + 2):
            self.arrived((6, k))
            self.start((6, k), 1)

    def finish(self):
        for piece, to in FORWARDS:
            self.copy(piece, to).wait_send()


def gate_up_kernel(tile, h_loc, w_gate, w_up, w_q, w_k, w_v, h_all, z_all, fa_all, fb_all, qkv_all, w_join,
                   hbuf, wg, wu, wq, z_st, fa_st, fb_st, qkv_st, send_sem, recv_sem, load_sem, w_sem, keep_sem, out_sem):
    step = pl.program_id(0)
    gather = Gather(hbuf, send_sem, recv_sem)
    width = wg.shape[1]
    tiles = width // tile

    def load(g):
        return pltpu.make_async_copy(h_loc.at[pl.ds(PIECES * g, PIECES)], hbuf.at[0, g], load_sem.at[g])

    def load_w(k, j):
        cols = pl.ds(j * tile, tile)
        src, dst = ((w_gate, wg), (w_up, wu))[k]
        return pltpu.make_async_copy(src.at[:, cols], dst.at[:, cols], w_sem.at[k, j])

    qrows, krows = w_q.shape[0], w_k.shape[0]
    load_q = [
        pltpu.make_async_copy(w_q, wq.at[pl.ds(0, qrows)], w_sem.at[2, 0]),
        pltpu.make_async_copy(w_k, wq.at[pl.ds(qrows, krows)], w_sem.at[2, 1]),
        pltpu.make_async_copy(w_v, wq.at[pl.ds(qrows + krows, krows)], w_sem.at[2, 2]),
    ]
    join = pltpu.make_async_copy(wq, w_join, w_sem.at[2, 3])

    def keep(u, p):
        rel, g = UNIT_PIECES[u][p]
        return pltpu.make_async_copy(hbuf.at[u, p], h_all.at[device_at(rel), pl.ds(PIECES * g, PIECES)], keep_sem.at[u, p])

    outs = ((z_st, z_all), (fa_st, fa_all), (fb_st, fb_all), (qkv_st, qkv_all))

    def put(u, k, p):
        rel, g = UNIT_PIECES[u][p]
        st, full = outs[k]
        return pltpu.make_async_copy(st.at[u % SLOTS, p], full.at[device_at(rel), pl.ds(PIECES * g, PIECES)], out_sem.at[u % SLOTS, k, p])

    def each(fn):
        for k in range(PIECES):
            for p in range(PIECES):
                fn(k, p)

    @pl.when(step == 0)
    def _():
        for g in range(PIECES):
            load(g).start()
        for j in range(tiles):
            load_w(0, j).start()
            load_w(1, j).start()
        for c in load_q:
            c.start()
        gather.greet()
        for g in range(PIECES):
            load(g).wait()
            for to in (2, PIECES, 1):
                gather.start((0, g), to)
            keep(0, g).start()

    @pl.when(step == 2)
    def _():
        for g in range(PIECES):
            gather.arrived((1, g))
            keep(1, g).start()

    for q in range(PIECES):
        @pl.when(step == 3 + 2 * q)
        def _():
            gather.pull(q)

        @pl.when(step == PIECES + 2 * q)
        def _():
            gather.arrived((3, q))
            gather.arrived((5, q))
            for p in range(PIECES):
                keep(2 + q, p).start()

    for g in range(2):
        @pl.when(step == 11 + 2 * g)
        def _():
            gather.pull_far(g)

        @pl.when(step == 12 + 2 * g)
        def _():
            gather.arrived((7, g))
            gather.arrived((7, g + 2))
            for p in range(PIECES):
                keep(6 + g, p).start()

    for u in range(2, DEVS):
        @pl.when(step == 2 * u)
        def _():
            each(lambda k, p: put(u - 2, k, p).wait())

    unit = step // SLOTS
    slot = lax.rem(unit, SLOTS)

    def rows_of(ref):
        x = ref[unit]
        return x.reshape(-1, x.shape[-1])

    def gate_up(j):
        @pl.when(step == 0 if j < 3 else step == 1)
        def _():
            load_w(0, j).wait()
            load_w(1, j).wait()
        cols = pl.ds(j * tile, tile)
        gate = jnp.dot(rows_of(hbuf), wg[:, cols], preferred_element_type=F32)
        up = jnp.dot(rows_of(hbuf), wu[:, cols], preferred_element_type=F32)
        sig = jax.nn.sigmoid(gate)
        act = gate * sig
        shape = z_st.shape[1:-1] + (tile,)
        z_st[slot, :, :, :, cols] = (act * up).astype(BF).reshape(shape)
        fa_st[slot, :, :, :, cols] = (up * sig * (1.0 + gate * (1.0 - sig))).reshape(shape)
        fb_st[slot, :, :, :, cols] = act.reshape(shape)

    @pl.when(lax.rem(step, SLOTS) == 0)
    def _():
        for j in range(3):
            gate_up(j)

    @pl.when(lax.rem(step, SLOTS) == 1)
    def _():
        for j in range(3, tiles):
            gate_up(j)

        @pl.when(step == 1)
        def _():
            for c in load_q:
                c.wait()
            join.start()
        qkv = lax.dot_general(rows_of(hbuf), wq[...], NT_DIMS, preferred_element_type=F32)
        qkv_st[slot] = qkv.reshape(qkv_st.shape[1:])

    for u in range(DEVS):
        @pl.when(step == 2 * u + 1)
        def _():
            each(lambda k, p: put(u, k, p).start())

    @pl.when(step == 15)
    def _():
        each(lambda k, p: put(6, k, p).wait())
        each(lambda k, p: put(7, k, p).wait())
        for u in range(DEVS):
            for p in range(PIECES):
                keep(u, p).wait()
        join.wait()
        gather.finish()


def gate_up_gather(h_loc, w_gate, w_up, w_q, w_k, w_v, tile=256):
    batch, local, width = h_loc.shape
    ffn, cols = w_gate.shape[1], w_q.shape[0] + w_k.shape[0] + w_v.shape[0]
    devs, quarter = DEVS, batch // PIECES
    tokens = devs * batch * local
    full = lambda c, t: jax.ShapeDtypeStruct((devs, batch, local, c), t)
    stage = lambda c, t: pltpu.VMEM((2, PIECES, quarter, local, c), t)
    return pl.pallas_call(
        functools.partial(gate_up_kernel, tile),
        grid=(16,),
        out_shape=(full(width, BF), full(ffn, BF), full(ffn, F32), full(ffn, F32), full(cols, F32), jax.ShapeDtypeStruct((cols, width), BF)),
        in_specs=[pl.BlockSpec(memory_space=pl.ANY)] * 6,
        out_specs=(pl.BlockSpec(memory_space=pl.ANY),) * 6,
        scratch_shapes=[
            pltpu.VMEM((DEVS, PIECES, quarter, local, width), BF),
            pltpu.VMEM(w_gate.shape, BF), pltpu.VMEM(w_up.shape, BF), pltpu.VMEM((cols, width), BF),
            stage(ffn, BF), stage(ffn, F32), stage(ffn, F32), stage(cols, F32),
            pltpu.SemaphoreType.DMA((len(FORWARDS),)),
            pltpu.SemaphoreType.DMA((DEVS, PIECES)),
            pltpu.SemaphoreType.DMA((PIECES,)),
            pltpu.SemaphoreType.DMA((3, ffn // tile)),
            pltpu.SemaphoreType.DMA((DEVS, PIECES)),
            pltpu.SemaphoreType.DMA((2, PIECES, PIECES)),
        ],
        compiler_params=pltpu.CompilerParams(collective_id=3, has_side_effects=True, vmem_limit_bytes=VMEM_LIMIT),
        cost_estimate=pl.CostEstimate(flops=2 * tokens * width * (2 * ffn + cols), bytes_accessed=tokens * (2 * width + 10 * ffn + PIECES * cols), transcendentals=0),
        name="gate_up_gather",
    )(h_loc, w_gate, w_up, w_q, w_k, w_v)


PLAN = ["y", "d", "y", "d", "y", "d", "y", "d", "y", "y", "d", "y", "y", "d", "d", "d"]
Y_STEPS = [i for i, k in enumerate(PLAN) if k == "y"]
D_STEPS = [i for i, k in enumerate(PLAN) if k == "d"]
PULL_STEPS = {PIECES: 0, 6: 1, 9: 2, 12: 3}


def place(step, steps):
    return sum(jnp.where(step == at, i, 0) for i, at in enumerate(steps))


def one_of(step, steps):
    hit = step == steps[0]
    for at in steps[1:]:
        hit = hit | (step == at)
    return hit


def branch_gather_kernel(tile, ytile, dy_loc, z_all, o_all, fa_all, fb_all, w_down, w_out,
                         dy_all, branch, dgate_all, dup_all, do_all,
                         buf, wd, wo, z_st, o_st, fa_st, fb_st, dgate_st, dup_st, do_st, y_st, y_in,
                         send_sem, recv_sem, load_sem, w_sem, keep_sem, out_sem, f_sem, a_sem, ysend_sem, yrecv_sem, yout_sem):
    step = pl.program_id(0)
    gather = Gather(buf, send_sem, recv_sem)
    ffn = wd.shape[0]
    me = lax.axis_index("tp")
    core = lax.rem(me, SLOTS)

    def load(g):
        return pltpu.make_async_copy(dy_loc.at[pl.ds(PIECES * g, PIECES)], buf.at[0, g], load_sem.at[g])

    load_w = [pltpu.make_async_copy(w_down, wd, w_sem.at[0]), pltpu.make_async_copy(w_out, wo, w_sem.at[1])]

    def keep(u, p):
        rel, g = UNIT_PIECES[u][p]
        return pltpu.make_async_copy(buf.at[u, p], dy_all.at[device_at(rel), pl.ds(PIECES * g, PIECES)], keep_sem.at[u, p])

    def factors(u):
        for p, (rel, g) in enumerate(UNIT_PIECES[u]):
            where = (device_at(rel), pl.ds(PIECES * g, PIECES))
            yield pltpu.make_async_copy(fa_all.at[where], fa_st.at[p], f_sem.at[0, p])
            yield pltpu.make_async_copy(fb_all.at[where], fb_st.at[p], f_sem.at[1, p])

    def results(u):
        for p, (rel, g) in enumerate(UNIT_PIECES[u]):
            where = (device_at(rel), pl.ds(PIECES * g, PIECES))
            yield pltpu.make_async_copy(dgate_st.at[p], dgate_all.at[where], out_sem.at[0, p])
            yield pltpu.make_async_copy(dup_st.at[p], dup_all.at[where], out_sem.at[1, p])
            yield pltpu.make_async_copy(do_st.at[p], do_all.at[where], out_sem.at[2, p])

    def y_loads(i):
        dev = 2 * (i % PIECES) + (1 - core if i < PIECES else core)
        yield pltpu.make_async_copy(z_all.at[dev], z_st.at[i % SLOTS], a_sem.at[i % SLOTS, 0])
        yield pltpu.make_async_copy(o_all.at[dev], o_st.at[i % SLOTS], a_sem.at[i % SLOTS, 1])

    def y_exchange(i):
        return pltpu.make_async_remote_copy(
            src_ref=y_st.at[i % SLOTS], dst_ref=y_in.at[i], send_sem=ysend_sem.at[i], recv_sem=yrecv_sem.at[i],
            device_id=(device_at(1),), device_id_type=pl.DeviceIdType.MESH)

    def y_out(i):
        return pltpu.make_async_copy(y_st.at[i % SLOTS], branch.at[i - PIECES], yout_sem.at[i % SLOTS])

    def start(copies):
        for c in copies:
            c.start()

    def wait(copies):
        for c in copies:
            c.wait()

    @pl.when(step == 0)
    def _():
        for g in range(PIECES):
            load(g).start()
        start(y_loads(0))
        start(load_w)
        start(y_loads(1))
        start(factors(0))
        gather.greet()
        for g in range(PIECES):
            load(g).wait()
            for to in (2, PIECES, 1):
                gather.start((0, g), to)
            keep(0, g).start()
        wait(load_w)

    for i, at in enumerate(Y_STEPS):
        @pl.when(step == at + 1)
        def _():
            if i < PIECES:
                y_exchange(i).start()
            else:
                y_out(i).start()
            if i + 2 < DEVS:
                start(y_loads(i + 2))

    for u, at in enumerate(D_STEPS[:-1]):
        @pl.when(step == at + 1)
        def _():
            start(results(u))
            start(factors(u + 1))

    for at, q in PULL_STEPS.items():
        @pl.when(step == at)
        def _():
            gather.pull(q)

    for u, at in enumerate(D_STEPS):
        @pl.when(step == at)
        def _():
            if u == 1:
                for g in range(PIECES):
                    gather.arrived((1, g))
            elif 2 <= u < 6:
                gather.arrived((3, u - 2))
                gather.arrived((5, u - 2))
            elif u >= 6:
                gather.pull_far(u - 6)
                gather.arrived((7, u - 6))
                gather.arrived((7, u - PIECES))
            if u > 0:
                for p in range(PIECES):
                    keep(u, p).start()
                wait(results(u - 1))
            wait(factors(u))

    for i, at in enumerate(Y_STEPS):
        @pl.when(step == at)
        def _():
            wait(y_loads(i))
            if 2 <= i < 6:
                y_exchange(i - 2).wait_send()
            elif i >= 6:
                y_out(i - 2).wait()
            if i >= PIECES:
                y_exchange(i - PIECES).wait_recv()

    y_index = place(step, Y_STEPS)
    unit = place(step, D_STEPS)
    y_slot = lax.rem(y_index, SLOTS)
    shape = y_st.shape[1:-1] + (ytile,)

    def y_product(t):
        cols = pl.ds(pl.multiple_of(t * ytile, ytile), ytile)
        z = z_st[y_slot].reshape(-1, ffn)
        o = o_st[y_slot].reshape(-1, wo.shape[0])
        prod = jnp.dot(z, wd[:, cols], preferred_element_type=F32) + jnp.dot(o, wo[:, cols], preferred_element_type=F32)
        return cols, prod

    @pl.when(one_of(step, Y_STEPS[:PIECES]))
    def _():
        @pl.loop(0, wd.shape[1] // ytile)
        def _(t):
            cols, prod = y_product(t)
            y_st[y_slot, :, :, cols] = prod.astype(BF).reshape(shape)

    @pl.when(one_of(step, Y_STEPS[PIECES:]))
    def _():
        @pl.loop(0, wd.shape[1] // ytile)
        def _(t):
            cols, prod = y_product(t)
            other = y_in[y_index - PIECES, :, :, cols].reshape(prod.shape)
            y_st[y_slot, :, :, cols] = (prod + other.astype(F32)).astype(BF).reshape(shape)

    @pl.when(one_of(step, D_STEPS))
    def _():
        def rows():
            x = buf[unit]
            return x.reshape(-1, x.shape[-1])

        for j in range(ffn // tile):
            cols = slice(j * tile, (j + 1) * tile)
            dz = lax.dot_general(rows(), wd[cols], NT_DIMS, preferred_element_type=F32)
            dz = dz.reshape(fa_st.shape[:-1] + (tile,))
            dgate_st[:, :, :, cols] = (dz * fa_st[:, :, :, cols]).astype(BF)
            dup_st[:, :, :, cols] = (dz * fb_st[:, :, :, cols]).astype(BF)
        do = lax.dot_general(rows(), wo[...], NT_DIMS, preferred_element_type=F32)
        do_st[...] = do.astype(BF).reshape(do_st.shape)

    @pl.when(step == len(PLAN) - 1)
    def _():
        start(results(7))
        y_out(6).wait()
        y_out(7).wait()
        for u in range(DEVS):
            for p in range(PIECES):
                keep(u, p).wait()
        gather.finish()
        wait(results(7))


def branch_gather(dy_loc, z_all, o_all, fa_all, fb_all, w_down, w_out, tile=256, ytile=1280):
    batch, local, width = dy_loc.shape
    devs, ffn, qcols = z_all.shape[0], z_all.shape[-1], o_all.shape[-1]
    quarter = batch // PIECES
    tokens = devs * batch * local
    full = lambda c: jax.ShapeDtypeStruct((devs, batch, local, c), BF)
    stage = lambda c, t: pltpu.VMEM((PIECES, quarter, local, c), t)
    dma = lambda *n: pltpu.SemaphoreType.DMA(n)
    return pl.pallas_call(
        functools.partial(branch_gather_kernel, tile, ytile),
        grid=(len(PLAN),),
        out_shape=(full(width), jax.ShapeDtypeStruct((devs // SLOTS, batch, local, width), BF), full(ffn), full(ffn), full(qcols)),
        in_specs=[pl.BlockSpec(memory_space=pl.ANY)] * 7,
        out_specs=(pl.BlockSpec(memory_space=pl.ANY),) * 5,
        scratch_shapes=[
            pltpu.VMEM((DEVS, PIECES, quarter, local, width), BF),
            pltpu.VMEM(w_down.shape, BF), pltpu.VMEM(w_out.shape, BF),
            pltpu.VMEM((2, batch, local, ffn), BF), pltpu.VMEM((2, batch, local, qcols), BF),
            stage(ffn, F32), stage(ffn, F32), stage(ffn, BF), stage(ffn, BF), stage(qcols, BF),
            pltpu.VMEM((2, batch, local, width), BF), pltpu.VMEM((PIECES, batch, local, width), BF),
            dma(len(FORWARDS)), dma(DEVS, PIECES), dma(PIECES), dma(2), dma(DEVS, PIECES), dma(3, PIECES), dma(2, PIECES), dma(2, 2), dma(PIECES), dma(PIECES), dma(2),
        ],
        compiler_params=pltpu.CompilerParams(collective_id=1, has_side_effects=True, vmem_limit_bytes=VMEM_LIMIT),
        cost_estimate=pl.CostEstimate(flops=PIECES * tokens * width * (ffn + qcols), bytes_accessed=tokens * (6 * width + 14 * ffn + PIECES * qcols), transcendentals=0),
        name="branch_gather",
    )(dy_loc, z_all, o_all, fa_all, fb_all, w_down, w_out)


class SmallSum:
    def __init__(self, part, out, pair_in, chip_sum, far_in, full, send_sem, recv_sem):
        self.part, self.out, self.pair_in, self.chip_sum, self.far_in, self.full = part, out, pair_in, chip_sum, far_in, full
        self.send_sem, self.recv_sem = send_sem, recv_sem
        self.me = lax.axis_index("tp")
        self.core, self.chip = lax.rem(self.me, 2), self.me // SLOTS

    def remote(self, src, dst, k, rel):
        return pltpu.make_async_remote_copy(
            src_ref=src, dst_ref=dst, send_sem=self.send_sem.at[k], recv_sem=self.recv_sem.at[k],
            device_id=(device_at(rel),), device_id_type=pl.DeviceIdType.MESH)

    def pair(self, j):
        return self.remote(self.part.at[2 * j + 1 - self.core], self.pair_in.at[j], j, 1)

    def far(self, k):
        rel = 2 * (k + 1)
        return self.remote(self.chip_sum.at[device_at(rel) // SLOTS], self.far_in.at[k], PIECES + k, rel)

    def share(self, rel):
        return self.remote(self.full.at[self.me], self.full.at[self.me], 6 + rel, rel)

    def on_step(self, step, last):
        @pl.when(step == 0)
        def _():
            for j in range(PIECES):
                self.pair(j).start()

        @pl.when(step == 2)
        def _():
            for j in range(PIECES):
                self.pair(j).wait_recv()
                self.chip_sum[j] = self.part[2 * j + self.core] + self.pair_in[j]

        @pl.when(step == 3)
        def _():
            for k in range(3):
                self.far(k).start()

        @pl.when(step == last - 6)
        def _():
            total = self.chip_sum[self.chip]
            for k in range(3):
                self.far(k).wait_recv()
                total += self.far_in[k]
            self.full[self.me] = total.astype(BF)

        @pl.when(step == last - 5)
        def _():
            for rel in PEERS:
                self.share(rel).start()

        @pl.when(step == last)
        def _():
            for rel in PEERS:
                self.share(rel).wait_recv()
            rows = self.full.shape[1]
            for d in range(DEVS):
                self.out[d // PIECES, d % PIECES * rows:(d % PIECES + 1) * rows] = self.full[d]
            for j in range(PIECES):
                self.pair(j).wait_send()
            for k in range(3):
                self.far(k).wait_send()
            for rel in PEERS:
                self.share(rel).wait_send()


def pair_matmul_kernel(num, trans, tiles, summed, *refs):
    a_hbm, b_refs = refs[:num], refs[num:2 * num]
    refs = refs[2 * num:]
    if summed:
        small_ref, out_ref, small_out = refs[:3]
        refs = refs[3:]
    else:
        out_ref, refs = refs[0], refs[1:]
    a_vmem = refs[:num]
    send_buf, recv_buf, a_sem, send_sem, recv_sem = refs[num:num + 5]
    step = pl.program_id(0)
    peers = PEERS if summed else (1,)
    me = lax.axis_index("tp")
    core = lax.rem(me, SLOTS)
    partner = me + 1 - 2 * core
    chips = a_vmem[0].shape[1]

    def load(half, which, chip):
        parity = 1 - core if half == 0 else core
        return pltpu.make_async_copy(a_hbm[which].at[chip, parity], a_vmem[which].at[half, chip], a_sem.at[half, which, chip])

    def exchange(tile):
        return pltpu.make_async_remote_copy(
            src_ref=send_buf.at[tile], dst_ref=recv_buf.at[tile], send_sem=send_sem.at[tile], recv_sem=recv_sem.at[tile],
            device_id=(partner,), device_id_type=pl.DeviceIdType.MESH)

    def product(half, rows):
        total = None
        for which in range(num):
            lhs = a_vmem[which][half, rows]
            lhs = lhs.reshape(-1, lhs.shape[-1])
            rhs = b_refs[which][...]
            term = lax.dot_general(lhs, rhs, NT_DIMS, preferred_element_type=F32) if trans[which] else jnp.dot(lhs, rhs, preferred_element_type=F32)
            total = term if total is None else total + term
        return total

    group = PIECES
    shape = (group,) + send_buf.shape[2:]

    @pl.when(step == 0)
    def _():
        for half in range(2):
            for which in range(num):
                for chip in range(chips):
                    load(half, which, chip).start()
        barrier = pltpu.get_barrier_semaphore()
        for rel in peers:
            pl.semaphore_signal(barrier, inc=1, device_id=(device_at(rel),), device_id_type=pl.DeviceIdType.MESH)
        pl.semaphore_wait(barrier, len(peers))

    if summed:
        SmallSum(small_ref, small_out, *refs[num + 5:]).on_step(step, 2 * tiles - 1)

    for tile in range(tiles):
        @pl.when(step == tile + 1)
        def _():
            exchange(tile).start()

    @pl.when(step == tiles)
    def _():
        for which in range(num):
            for chip in range(chips):
                load(1, which, chip).wait()

    for tile in range(tiles):
        @pl.when(step == tile + tiles)
        def _():
            exchange(tile).wait_recv()

    @pl.when(step < tiles)
    def _():
        @pl.loop(0, chips // group)
        def _(g):
            @pl.when(step == 0)
            def _():
                for which in range(num):
                    for chip in range(group):
                        load(0, which, g * group + chip).wait()
            rows = pl.ds(g * group, group)
            send_buf[step, rows] = product(0, rows).astype(BF).reshape(shape)

    @pl.when(step >= tiles)
    def _():
        @pl.loop(0, chips // group)
        def _(g):
            rows = pl.ds(g * group, group)
            arrived = recv_buf[step - tiles, rows].reshape(-1, shape[-1])
            out_ref[rows] = (product(1, rows) + arrived.astype(F32)).astype(BF).reshape(shape)

    @pl.when(step == 2 * tiles - 1)
    def _():
        for tile in range(tiles):
            exchange(tile).wait_send()


def pair_matmul(lhs, rhs, trans, collective_id, name, tile=512, small=None):
    num = len(lhs)
    devs, batch, local = lhs[0].shape[:3]
    chips, seq = devs // SLOTS, devs * local
    lhs = [a.reshape(chips, 2, batch, local, a.shape[-1]) for a in lhs]
    width = rhs[0].shape[0] if trans[0] else rhs[0].shape[1]
    tiles = width // tile
    in_specs = [pl.BlockSpec(memory_space=pl.ANY)] * num
    for b, t in zip(rhs, trans):
        if t:
            in_specs.append(pl.BlockSpec((tile, b.shape[1]), lambda i: (lax.rem(i, tiles), 0)))
        else:
            in_specs.append(pl.BlockSpec((b.shape[0], tile), lambda i: (0, lax.rem(i, tiles))))
    depth = sum(a.shape[-1] for a in lhs)
    out_shape = [jax.ShapeDtypeStruct((chips, batch, local, width), BF)]
    out_specs = [pl.BlockSpec((chips, batch, local, tile), lambda i: (0, 0, 0, lax.max(i - tiles, 0)))]
    scratch = [pltpu.VMEM((2, chips, batch, local, a.shape[-1]), BF) for a in lhs] + [
        pltpu.VMEM((tiles, chips, batch, local, tile), BF),
        pltpu.VMEM((tiles, chips, batch, local, tile), BF),
        pltpu.SemaphoreType.DMA((2, num, chips)),
        pltpu.SemaphoreType.DMA((tiles,)),
        pltpu.SemaphoreType.DMA((tiles,)),
    ]
    extra = []
    if small is not None:
        extra = [small]
        _, rows, cols = small.shape
        in_specs.append(pl.BlockSpec(small.shape, lambda i: (0, 0, 0), pipeline_mode=pl.Buffered(1)))
        joined = (DEVS // PIECES, PIECES * rows, cols)
        out_shape.append(jax.ShapeDtypeStruct(joined, BF))
        out_specs.append(pl.BlockSpec(joined, lambda i: (0, 0, 0), pipeline_mode=pl.Buffered(1)))
        scratch += [pltpu.VMEM((PIECES, rows, cols), F32), pltpu.VMEM((PIECES, rows, cols), F32), pltpu.VMEM((3, rows, cols), F32),
                    pltpu.VMEM((DEVS, rows, cols), BF), pltpu.SemaphoreType.DMA((14,)), pltpu.SemaphoreType.DMA((14,))]
    outs = pl.pallas_call(
        functools.partial(pair_matmul_kernel, num, trans, tiles, small is not None),
        grid=(2 * tiles,),
        out_shape=out_shape,
        in_specs=in_specs,
        out_specs=out_specs,
        scratch_shapes=scratch,
        compiler_params=pltpu.CompilerParams(collective_id=collective_id, has_side_effects=True, vmem_limit_bytes=VMEM_LIMIT),
        cost_estimate=pl.CostEstimate(flops=2 * batch * seq * width * depth, bytes_accessed=2 * depth * (batch * seq + width), transcendentals=0),
        name=name,
    )(*lhs, *rhs, *extra)
    return outs[0] if small is None else outs


ROWS = 16


def norm_kernel(x_ref, gain_ref, h_ref):
    per = x_ref.shape[1] // ROWS

    def rows_step(t, carry):
        where = (t // per, pl.ds(pl.multiple_of(lax.rem(t, per) * ROWS, ROWS), ROWS))
        x = x_ref[where].astype(F32)
        centered = x - row_mean(x)
        inv_std = lax.rsqrt(row_mean(centered * centered) + LN_EPS)
        h_ref[where] = (gain_ref[...] * (centered * inv_std)).astype(BF)
        return carry

    lax.fori_loop(0, x_ref.shape[0] * per, rows_step, 0, unroll=PIECES)


def norm(x, gain, rows=DEVS):
    batch, local, width = x.shape
    block = pl.BlockSpec((rows, local, width), lambda b: (b, 0, 0))
    return pl.pallas_call(
        norm_kernel,
        grid=(batch // rows,),
        out_shape=jax.ShapeDtypeStruct(x.shape, BF),
        in_specs=[block, pl.BlockSpec((width,), lambda b: (0,))],
        out_specs=block,
        compiler_params=pltpu.CompilerParams(vmem_limit_bytes=VMEM_LIMIT),
        name="norm",
    )(x, gain)


def finish_kernel(steps, x_ref, dh_ref, dy_ref, gain_ref, dx_ref, dgain_ref, acc, parts, send_sem, recv_sem):
    step = pl.program_id(0)
    me = lax.axis_index("tp")
    barrier = pltpu.get_barrier_semaphore()

    def share(rel):
        return pltpu.make_async_remote_copy(
            src_ref=parts.at[me], dst_ref=parts.at[me], send_sem=send_sem.at[rel], recv_sem=recv_sem.at[rel],
            device_id=(device_at(rel),), device_id_type=pl.DeviceIdType.MESH)

    @pl.when(step == 0)
    def _():
        acc[...] = jnp.zeros_like(acc)
        for rel in PEERS:
            pl.semaphore_signal(barrier, inc=1, device_id=(device_at(rel),), device_id_type=pl.DeviceIdType.MESH)

    per = x_ref.shape[1] // ROWS

    def rows_step(t, carry):
        where = (t // per, pl.ds(pl.multiple_of(lax.rem(t, per) * ROWS, ROWS), ROWS))
        x = x_ref[where].astype(F32)
        centered = x - row_mean(x)
        inv_std = lax.rsqrt(row_mean(centered * centered) + LN_EPS)
        x_hat = centered * inv_std
        dh = dh_ref[where].astype(F32)
        prod = dh * x_hat
        acc[...] += prod[:DEVS] + prod[DEVS:]
        grad_hat = dh * gain_ref[...]
        mean_hat = row_mean(grad_hat)
        mean_dot = row_mean(grad_hat * x_hat)
        dx_ref[where] = (inv_std * (grad_hat - mean_hat - x_hat * mean_dot) + dy_ref[where].astype(F32)).astype(BF)
        return carry

    lax.fori_loop(0, x_ref.shape[0] * per, rows_step, 0, unroll=PIECES)

    @pl.when(step == steps - 1)
    def _():
        parts[me] = jnp.sum(acc[...], axis=0, keepdims=True)
        pl.semaphore_wait(barrier, 7)
        for rel in PEERS:
            share(rel).start()
        for rel in PEERS:
            share(rel).wait_recv()
        total = parts[0]
        for d in PEERS:
            total += parts[d]
        dgain_ref[...] = total.reshape(-1)
        for rel in PEERS:
            share(rel).wait_send()


def finish(x, dh, dy, gain, rows=DEVS):
    batch, local, width = x.shape
    steps = batch // rows
    block = pl.BlockSpec((rows, local, width), lambda b: (b, 0, 0))
    return pl.pallas_call(
        functools.partial(finish_kernel, steps),
        grid=(steps,),
        out_shape=(jax.ShapeDtypeStruct(x.shape, BF), jax.ShapeDtypeStruct((width,), F32)),
        in_specs=[block, block, block, pl.BlockSpec((width,), lambda b: (0,))],
        out_specs=(block, pl.BlockSpec((width,), lambda b: (0,))),
        scratch_shapes=[pltpu.VMEM((DEVS, width), F32), pltpu.VMEM((DEVS, 1, width), F32), pltpu.SemaphoreType.DMA((DEVS,)), pltpu.SemaphoreType.DMA((DEVS,))],
        compiler_params=pltpu.CompilerParams(collective_id=PIECES, has_side_effects=True, vmem_limit_bytes=VMEM_LIMIT),
        name="finish",
    )(x, dh, dy, gain)


def solution(mesh):
    group_size = mesh.shape["tp"]
    same_core = [[c + 2 * j for j in range(group_size // SLOTS)] for c in range(2)]

    def layer_shard(x_loc, grad_y_loc, ln_gain, w_query, w_key, w_value, w_out, w_gate, w_up, w_down):
        head_dim = w_key.shape[1]
        heads = w_query.shape[1]
        width = x_loc.shape[2]
        seq_len = x_loc.shape[1] * group_size
        cos_tab, sin_tab = rope_tables(seq_len, head_dim)
        w_query_t = w_query.transpose(1, 2, 0).reshape(heads * head_dim, width)
        w_out_2d = w_out.reshape(heads * head_dim, width)

        normed_loc = norm(x_loc, ln_gain)
        normed, hidden, gate_factor, gate_act, qkv, w_qkv_t = gate_up_gather(normed_loc, w_gate, w_up, w_query_t, w_key.T, w_value.T)

        attn, rot, stat = attn_fwd(qkv, cos_tab, sin_tab, heads)
        grad, branch, grad_gate, grad_up, grad_heads = branch_gather(grad_y_loc, hidden, attn, gate_factor, gate_act, w_down, w_out_2d)
        y_sum = lax.psum_scatter(branch, "tp", scatter_dimension=0, tiled=False, axis_index_groups=same_core)

        dqkv = attn_bwd(rot, grad_heads, stat, cos_tab, sin_tab, heads)
        dw_qkv = jnp.einsum("zblk,zbld->kd", dqkv, normed, preferred_element_type=F32)
        kv_part = dw_qkv[heads * head_dim:].reshape(DEVS, head_dim // PIECES, width)
        dw_query, kv_part = lax.optimization_barrier((dw_qkv[:heads * head_dim].astype(BF), kv_part))
        dh_part, dw_kv = pair_matmul([grad_gate, grad_up, dqkv], [w_gate, w_up, w_qkv_t], (True, True, False), 2, "dh_mm", tile=256, small=kv_part)
        dh_part, y_sum, normed, grad = lax.optimization_barrier((dh_part, y_sum, normed, grad))
        dh_sum = lax.psum_scatter(dh_part, "tp", scatter_dimension=0, tiled=False, axis_index_groups=same_core)

        total = lambda spec, a, b: jnp.einsum(spec, a, b, preferred_element_type=F32)
        dw_query = dw_query.reshape(heads, head_dim, width).transpose(2, 0, 1)
        dw_out = total("zblk,zbld->kd", attn, grad).reshape(heads, head_dim, width)
        dw_down = total("zblf,zbld->fd", hidden, grad)
        dw_gate = total("zbld,zblf->df", normed, grad_gate)
        dw_up = total("zbld,zblf->df", normed, grad_up)

        dx, dgain = finish(x_loc, dh_sum, grad_y_loc, ln_gain)
        return (
            (x_loc.astype(F32) + y_sum.astype(F32)).astype(BF),
            dx,
            dgain,
            dw_query,
            dw_kv[0].T,
            dw_kv[1].T,
            dw_out.astype(BF),
            dw_gate.astype(BF),
            dw_up.astype(BF),
            dw_down.astype(BF),
        )

    act_spec = P(None, "tp", None)
    weight_specs = (P(), P(None, "tp", None), P(), P(), P("tp", None, None), P(None, "tp"), P(None, "tp"), P("tp", None))
    return jax.shard_map(layer_shard, mesh=mesh, in_specs=(act_spec, act_spec) + weight_specs, out_specs=(act_spec, act_spec) + weight_specs, check_vma=False)
```
